32 devices in a mesh: gz: 4 (over z), gy: 2 (over y), gx: 4 (over x, core).
Axes of the slice: x: 2, y: 2, z: 4, core: 2. Of those that a mesh axis runs over, the one named last changes fastest.
Arguments:
- velocity: float32 [3, 128, 32, 512], P(None, 'gx', 'gy', 'gz'), may hold values from -3.5 to 5.5
- pressure: float32 [128, 32, 512], P('gx', 'gy', 'gz'), may hold values from -6 to 6
- voidage: float32 [128, 32, 512], P('gx', 'gy', 'gz'), may hold values from 0.5 to 0.95
- particle_vel: float32 [3, 128, 32, 512], P(None, 'gx', 'gy', 'gz'), may hold values from -6 to 6
- forcing: float32 [1], replicated, may hold values from 0.5 to 2
- target_flux: float32 [1], replicated, may hold values from 0.5 to 1.5
Outputs:
- vel_new: float32 [3, 128, 32, 512], P(None, 'gx', 'gy', 'gz')
- source: float32 [128, 32, 512], P('gx', 'gy', 'gz')
- forcing_new: float32 [1], replicated
The draws below stay inside these ranges and needn't reach their ends.
All inputs are finite; a program needn't handle non-finite values.
Results may differ from the reference program's by a relative error of at most 0.000079.
Values sent between devices are 32-bit elements; how exact they have to be, the bound alone decides.
No kernel may reach another device: no remote copies, remote signals or barrier semaphores. Data moves between devices by JAX's collectives and lax.ppermute only.
A program may use at most 64 MiB of HBM per device.

```python
import jax
import jax.numpy as jnp
from jax import lax

NX = 128
NY = 32
NZ = 512


def draw_velocity(key, part):
    jitter_field = jnp.clip(jax.random.normal(key, (3, NX, NY, NZ), jnp.float32), -3.5, 3.5)
    mean_lift = 2.0
    upward_mask = (jnp.arange(3) == 2).astype(jnp.float32).reshape(3, 1, 1, 1)
    return (jitter_field + mean_lift * upward_mask).astype(jnp.float32)


def levels(stream_key, shape, split, low, top_value):
    factor_of = 1.0
    for dim, shards_of in split:
        draws = jax.random.uniform(jax.random.fold_in(jax.random.fold_in(stream_key, 6), dim), (shards_of,), jnp.float32, low / len(split), top_value / len(split))
        factor_of = factor_of * jnp.repeat(jnp.exp(draws), shape[dim] // shards_of).reshape((-1,) + (1,) * (len(shape) - 1 - dim))
    return factor_of


def noise(key, extent, deviation, reach, split=(), kind=jnp.bfloat16):
    result = jax.random.normal(key, extent, jnp.float32) * deviation
    if len(split) > 0:
        result = levels(key, extent, split, -0.22, 0.18) * result
    return jnp.clip(result, min=-reach, max=reach).astype(kind)


def setup_inputs(seed: int = 0) -> dict:
    seeds = jax.random.split(jax.random.key(seed), 7)
    velocity = draw_velocity(jax.random.fold_in(seeds[6], 71), 0)
    pressure = noise(seeds[1], (NX, NY, NZ), 1.0, 6.0, ((0, 4), (1, 2), (2, 4)), jnp.float32)
    voidage = jnp.clip(0.5 + 0.45 * jax.random.uniform(seeds[2], (NX, NY, NZ), jnp.float32) ** levels(seeds[2], (NX, NY, NZ), ((0, 4), (1, 2), (2, 4)), -0.2, 0.2), 0.5, 0.95)
    particle_vel = noise(seeds[3], (3, NX, NY, NZ), 1.0, 6.0, ((1, 4), (2, 2), (3, 4)), jnp.float32)
    forcing = jnp.clip(jax.random.uniform(seeds[4], (1,), jnp.float32, 0.5, 2.0), 0.5, 2.0)
    target_flux = jnp.clip(jax.random.uniform(seeds[5], (1,), jnp.float32, 0.5, 1.5), 0.5, 1.5)
    return {"velocity": velocity, "pressure": pressure, "voidage": voidage, "particle_vel": particle_vel, "forcing": forcing, "target_flux": target_flux}


time_step = 0.2
viscosity = 0.1
drag_scale = 1.0

def shifted(field, axis_no, offset):
    slices = [slice(1, -1)] * 3
    length = field.shape[field.ndim - 3 + axis_no]
    slices[axis_no] = slice(1 + offset, length - 1 + offset)
    return field[tuple([slice(None)] * (field.ndim - 3) + slices)]

def upward():
    return (jnp.arange(3) == 2).astype(jnp.float32).reshape(3, 1, 1, 1)

def predict(vel_pad, pres_pad, voidage, particle_vel, forcing):
    centre = shifted(vel_pad, 0, 0)
    advection = jnp.zeros_like(centre)
    laplace = -6.0 * centre
    grads = []
    for axis_no in range(3):
        upper = shifted(vel_pad, axis_no, 1)
        lower = shifted(vel_pad, axis_no, -1)
        advection = advection + centre[axis_no] * (upper - lower) * 0.5
        laplace = laplace + upper + lower
        grads.append((shifted(pres_pad, axis_no, 1) - shifted(pres_pad, axis_no, -1)) * 0.5)
    forces = -advection + viscosity * laplace - jnp.stack(grads) + forcing * upward()
    slip_speed = jnp.sqrt(lax.optimization_barrier(jnp.sum((centre - particle_vel) ** 2, axis=0)))
    drag_rate = drag_scale * (1.0 - voidage) * voidage ** (-2.65) * (1.0 + slip_speed)
    return (centre + time_step * (forces + drag_rate * particle_vel)) / (1.0 + time_step * drag_rate)

def reference(velocity, pressure, voidage, particle_vel, forcing, target_flux):
    vel_pad = jnp.pad(velocity, ((0, 0), (1, 1), (1, 1), (0, 0)))
    vel_pad = jnp.pad(vel_pad, ((0, 0), (0, 0), (0, 0), (1, 1)), mode='wrap')
    pres_pad = jnp.pad(pressure, ((0, 0), (0, 0), (1, 1)), mode='wrap')
    pres_pad = jnp.pad(pres_pad, ((1, 1), (1, 1), (0, 0)), mode='edge')
    ustar = predict(vel_pad, pres_pad, voidage, particle_vel, forcing[0])
    flow_sum = jnp.sum(voidage * ustar[2])
    void_sum = jnp.sum(voidage)
    cells = voidage.size
    force_step = (target_flux[0] * cells - flow_sum) / (time_step * void_sum)
    vel_new = ustar + time_step * force_step * upward()
    flux = voidage * vel_new
    flux_pad = jnp.pad(flux, ((0, 0), (1, 1), (1, 1), (0, 0)))
    flux_pad = jnp.pad(flux_pad, ((0, 0), (0, 0), (0, 0), (1, 1)), mode='wrap')
    source = jnp.zeros_like(voidage)
    for axis_no in range(3):
        source = source + (shifted(flux_pad[axis_no], axis_no, 1) - shifted(flux_pad[axis_no], axis_no, -1)) * 0.5
    return (vel_new, source, forcing + force_step)
```

```python
import functools
import math

import jax
import jax.numpy as jnp
from jax import lax
from jax.experimental import pallas as pl
from jax.experimental.pallas import tpu as pltpu
from jax.sharding import PartitionSpec as P

time_step = 0.2
viscosity = 0.1
drag_scale = 1.0

PARAMS = pltpu.CompilerParams(vmem_limit_bytes=16 * 2**20)


def pairs_a(count):
    return [(i, i ^ 1) for i in range(count)]


def pairs_b(count):
    swaps = []
    for i in range(1, count, 2):
        swaps += [(i, (i + 1) % count), ((i + 1) % count, i)]
    return swaps


def even(axis):
    return lax.axis_index(axis) % 2 == 0


def z_rows(field):
    return field.T


def pack_kernel(vel, pres, void, x_a, x_b, y_a, y_b, z_a, z_b, columns):
    _, nx, ny, nz = vel.shape
    x_even, y_even, z_even = even("gx"), even("gy"), even("gz")
    for out, at in ((x_a, jnp.where(x_even, nx - 1, 0)), (x_b, jnp.where(x_even, 0, nx - 1))):
        for c in range(3):
            out[c] = vel[c, at]
        out[3] = pres[at]
    at_a, at_b = jnp.where(y_even, ny - 1, 0), jnp.where(y_even, 0, ny - 1)
    lane = lax.broadcasted_iota(jnp.int32, (ny, nz), 1)

    def slab(i, carry):
        for out, at in ((y_a, at_a), (y_b, at_b)):
            if out is not None:
                for c in range(3):
                    out[c, pl.ds(i, 1), :] = vel[c, i, pl.ds(at, 1), :]
                out[3, pl.ds(i, 1), :] = pres[i, pl.ds(at, 1), :]
        fields = [vel[0, i], vel[1, i], vel[2, i], pres[i], void[i]]
        joined = pltpu.roll(fields[0], 1, 1)
        for f in range(1, 5):
            joined = jnp.where(lane >= 2 * f, pltpu.roll(fields[f], 2 * f + 1, 1), joined)
        columns[pl.ds(pl.multiple_of(i * ny, ny), ny), :] = joined
        return carry

    lax.fori_loop(0, nx, slab, 0, unroll=4)
    rows = z_rows(columns[...])
    for f in range(5):
        high, low = rows[2 * f : 2 * f + 1], rows[2 * f + 1 : 2 * f + 2]
        z_a[f : f + 1, :] = jnp.where(z_even, high, low)
        z_b[f : f + 1, :] = jnp.where(z_even, low, high)
    for out in (z_a, z_b):
        out[5:8, :] = jnp.zeros((3, out.shape[1]), jnp.float32)


def predict_kernel(
    forcing, vel, pres, void, part, x_a, x_b, y_a, y_b, z_a, z_b,
    ustar, slope, fx_a, fx_b, fy_a, fy_b, fz_a, fz_b, sums, halo, columns,
):
    _, nx, ny, nz = vel.shape
    x_even, y_even, z_even = even("gx"), even("gy"), even("gz")
    xi, yi = lax.axis_index("gx"), lax.axis_index("gy")
    x_low, x_high = xi == 0, xi == lax.axis_size("gx") - 1
    y_low, y_high = yi == 0, yi == lax.axis_size("gy") - 1
    low_rows = jnp.where(z_even, z_b[...], z_a[...])
    high_rows = jnp.where(z_even, z_a[...], z_b[...])
    halo[...] = jnp.concatenate(
        [low_rows, high_rows, jnp.zeros((nz - 16, low_rows.shape[1]), jnp.float32)], axis=0
    ).T
    lane = lax.broadcasted_iota(jnp.int32, (ny, nz), 1)
    row = lax.broadcasted_iota(jnp.int32, (ny, nz), 0)
    forcing_now = forcing[0]
    y_at_a, y_at_b = jnp.where(y_even, ny - 1, 0), jnp.where(y_even, 0, ny - 1)

    def load(f, i):
        return vel[f, i] if f < 3 else pres[i]

    def x_low_halo(f):
        wall = 0.0 if f < 3 else pres[0]
        return jnp.where(x_low, wall, jnp.where(x_even, x_b[f], x_a[f]))

    def x_high_halo(f):
        wall = 0.0 if f < 3 else pres[nx - 1]
        return jnp.where(x_high, wall, jnp.where(x_even, x_a[f], x_b[f]))

    def slab(i, first, last, acc):
        rows_at = pl.ds(i * ny if isinstance(i, int) else pl.multiple_of(i * ny, ny), ny)
        edge = halo[rows_at, :]
        sides = []
        for f in range(4):
            here = load(f, i)
            xm = x_low_halo(f) if first else load(f, i - 1)
            xp = x_high_halo(f) if last else load(f, i + 1)
            row_a = y_a[f, pl.ds(i, 1), :]
            row_b = y_b[f, pl.ds(i, 1), :] if y_b is not None else row_a
            wall_m = 0.0 if f < 3 else here[0:1]
            wall_p = 0.0 if f < 3 else here[ny - 1 : ny]
            ym_row = jnp.where(y_low, wall_m, jnp.where(y_even, row_b, row_a))
            yp_row = jnp.where(y_high, wall_p, jnp.where(y_even, row_a, row_b))
            ym = jnp.where(row == 0, ym_row, pltpu.roll(here, 1, 0))
            yp = jnp.where(row == ny - 1, yp_row, pltpu.roll(here, ny - 1, 0))
            zm = jnp.where(lane == 0, edge[:, f : f + 1], pltpu.roll(here, 1, 1))
            zp = jnp.where(lane == nz - 1, edge[:, 8 + f : 9 + f], pltpu.roll(here, nz - 1, 1))
            sides.append((here, xm, xp, ym, yp, zm, zp))
        eps = void[i]
        em = jnp.where(lane == 0, edge[:, 4:5], pltpu.roll(eps, 1, 1))
        ep = jnp.where(lane == nz - 1, edge[:, 12:13], pltpu.roll(eps, nz - 1, 1))
        slope[i] = (ep - em) * 0.5
        u = [sides[c][0] for c in range(3)]
        pv = [part[c, i] for c in range(3)]
        slip2 = (u[0] - pv[0]) ** 2 + (u[1] - pv[1]) ** 2 + (u[2] - pv[2]) ** 2
        rate = (
            drag_scale * (1.0 - eps) * jnp.exp(-2.65 * jnp.log(eps)) * (1.0 + jnp.sqrt(slip2))
        )
        scale = 1.0 / (1.0 + time_step * rate)
        out = []
        for c in range(3):
            here, xm, xp, ym, yp, zm, zp = sides[c]
            advection = (u[0] * (xp - xm) + u[1] * (yp - ym) + u[2] * (zp - zm)) * 0.5
            laplace = xm + xp + ym + yp + zm + zp - 6.0 * here
            grad = (sides[3][2 + 2 * c] - sides[3][1 + 2 * c]) * 0.5
            force = viscosity * laplace - advection - grad
            if c == 2:
                force = force + forcing_now
            value = (here + time_step * (force + rate * pv[c])) * scale
            ustar[c, i] = value
            out.append(eps * value)
        fy_a[pl.ds(i, 1), :] = jnp.where(y_even, out[1][ny - 1 : ny], out[1][0:1])
        if fy_b is not None:
            fy_b[pl.ds(i, 1), :] = jnp.where(y_even, out[1][0:1], out[1][ny - 1 : ny])
        columns[rows_at, :] = out[2]
        if first:
            fx_b[...] = out[0]
        if last:
            fx_a[0:ny] = out[0]
        return acc[0] + out[2], acc[1] + eps

    zero = jnp.zeros((ny, nz), jnp.float32)
    acc = slab(0, True, False, (zero, zero))
    acc = lax.fori_loop(1, nx - 1, lambda i, a: slab(i, False, False, a), acc, unroll=2)
    flow, total = slab(nx - 1, False, True, acc)
    high, low = fx_a[0:ny], fx_b[...]
    fx_a[0:ny] = jnp.where(x_even, high, low)
    fx_b[...] = jnp.where(x_even, low, high)
    both = jnp.concatenate(
        [
            functools.reduce(jnp.add, [v[8 * k : 8 * k + 8] for k in range(ny // 8)])
            for v in (flow, total)
        ],
        axis=0,
    )
    fx_a[ny : ny + 16] = both
    sums[...] = both
    turned = z_rows(columns[...])
    z_low, z_high = turned[0:1], turned[nz - 1 : nz]
    send_a, send_b = jnp.where(z_even, z_high, z_low), jnp.where(z_even, z_low, z_high)
    for out, send in ((fz_a, send_a), (fz_b, send_b)):
        out[...] = jnp.broadcast_to(send, out.shape)


def divergence_kernel(void, ustar, div):
    _, nx, ny, nz = ustar.shape
    lane = lax.broadcasted_iota(jnp.int32, (ny, nz), 1)
    row = lax.broadcasted_iota(jnp.int32, (ny, nz), 0)

    def slab(i, first, last):
        eps = void[i]
        zero = jnp.zeros((ny, nz), jnp.float32)
        xm = zero if first else void[i - 1] * ustar[0, i - 1]
        xp = zero if last else void[i + 1] * ustar[0, i + 1]
        fy, fz = eps * ustar[1, i], eps * ustar[2, i]
        ym = jnp.where(row == 0, 0.0, pltpu.roll(fy, 1, 0))
        yp = jnp.where(row == ny - 1, 0.0, pltpu.roll(fy, ny - 1, 0))
        zm = jnp.where(lane == 0, 0.0, pltpu.roll(fz, 1, 1))
        zp = jnp.where(lane == nz - 1, 0.0, pltpu.roll(fz, nz - 1, 1))
        div[i] = ((xp - xm) + (yp - ym) + (zp - zm)) * 0.5

    slab(0, True, False)

    def step(i, carry):
        slab(i, False, False)
        return carry

    lax.fori_loop(1, nx - 1, step, 0, unroll=2)
    slab(nx - 1, False, True)


def finish_kernel(
    cells, forcing, target, uz, div, slope, sums, fx_a, fx_b, fy_a, fy_b, fz_a, fz_b,
    vel_new, source, forcing_new, halo,
):
    nx, ny, nz = div.shape
    x_even, y_even, z_even = even("gx"), even("gy"), even("gz")
    xi, yi = lax.axis_index("gx"), lax.axis_index("gy")
    x_low, x_high = xi == 0, xi == lax.axis_size("gx") - 1
    y_low, y_high = yi == 0, yi == lax.axis_size("gy") - 1
    flow, total = jnp.sum(sums[0:8]), jnp.sum(sums[8:16])
    step = (target[0] * cells - flow) / (time_step * total)
    forcing_new[0] = forcing[0] + step
    rise = time_step * step
    a, b = fz_a[0:1, 0 : nx * ny], fz_b[0:1, 0 : nx * ny]
    low_row, high_row = jnp.where(z_even, b, a), jnp.where(z_even, a, b)
    pick = lax.broadcasted_iota(jnp.int32, (nz, halo.shape[0]), 0)
    halo[...] = jnp.where(pick == 0, -low_row, jnp.where(pick == nz - 1, high_row, 0.0)).T
    xl = jnp.where(x_low, 0.0, jnp.where(x_even, fx_b[0:ny], fx_a[0:ny]))
    xh = jnp.where(x_high, 0.0, jnp.where(x_even, fx_a[0:ny], fx_b[0:ny]))
    row = lax.broadcasted_iota(jnp.int32, (ny, nz), 0)

    def slab(i, carry):
        rows_at = pl.ds(pl.multiple_of(i * ny, ny), ny)
        row_a = fy_a[pl.ds(i, 1), :]
        row_b = fy_b[pl.ds(i, 1), :] if fy_b is not None else row_a
        ym = jnp.where(y_low, 0.0, jnp.where(y_even, row_b, row_a))
        yp = jnp.where(y_high, 0.0, jnp.where(y_even, row_a, row_b))
        ends = jnp.where(row == 0, -ym, jnp.where(row == ny - 1, yp, 0.0)) + halo[rows_at, :]
        source[i] = div[i] + 0.5 * ends + rise * slope[i]
        vel_new[0, i] = uz[0, i] + rise
        return carry

    lax.fori_loop(0, nx, slab, 0, unroll=4)
    source[0] = source[0] - 0.5 * xl
    source[nx - 1] = source[nx - 1] + 0.5 * xh


def swap(value, axis, second=False):
    count = lax.axis_size(axis)
    return lax.ppermute(value, axis, pairs_b(count) if second else pairs_a(count))


def optional(kernel, slots):
    def run(*refs):
        refs = list(refs)
        for slot in slots:
            refs.insert(slot, None)
        return kernel(*refs)

    return run


def f32(*shape):
    return jax.ShapeDtypeStruct(shape, jnp.float32)


def local(velocity, pressure, voidage, particle_vel, forcing, target_flux):
    _, nx, ny, nz = velocity.shape
    counts = {axis: lax.axis_size(axis) for axis in ("gx", "gy", "gz")}
    cells = float(voidage.size * math.prod(counts.values()))
    two_y = counts["gy"] > 2
    flat = nx * ny
    smem = pl.BlockSpec(memory_space=pltpu.SMEM)
    vmem = pl.BlockSpec(memory_space=pltpu.VMEM)

    y_out = [f32(4, nx, nz)] * (2 if two_y else 1)
    faces = pl.pallas_call(
        optional(pack_kernel, () if two_y else (6,)),
        out_shape=[f32(4, ny, nz), f32(4, ny, nz)] + y_out + [f32(8, flat), f32(8, flat)],
        in_specs=[vmem] * 3,
        scratch_shapes=[pltpu.VMEM((flat, nz), jnp.float32)],
        compiler_params=PARAMS,
        name="pack",
    )(velocity, pressure, voidage)
    x_a, x_b, *y_faces, z_a, z_b = faces
    got = [swap(x_a, "gx"), swap(x_b, "gx", True)]
    got += [swap(y, "gy", k == 1) for k, y in enumerate(y_faces)]
    got += [swap(z_a, "gz"), swap(z_b, "gz", True)]

    ustar, slope, fx_a, fx_b, *fy, fz_a, fz_b, sums = pl.pallas_call(
        optional(predict_kernel, () if two_y else (8, 16)),
        out_shape=[f32(3, nx, ny, nz), f32(nx, ny, nz), f32(ny + 16, nz), f32(ny, nz)]
        + [f32(nx, nz)] * (2 if two_y else 1)
        + [f32(8, flat), f32(8, flat), f32(16, nz)],
        in_specs=[smem] + [vmem] * (4 + len(got)),
        scratch_shapes=[pltpu.VMEM((flat, nz), jnp.float32)] * 2,
        compiler_params=PARAMS,
        name="predict",
    )(forcing, velocity, pressure, voidage, particle_vel, *got)

    div = pl.pallas_call(
        divergence_kernel,
        out_shape=f32(nx, ny, nz),
        in_specs=[vmem] * 2,
        compiler_params=PARAMS,
        name="divergence",
    )(voidage, ustar)

    def stage(value, total, axis, second, adds):
        got_here = swap(value, axis, second)
        if adds:
            total = total + got_here[-16:, :nz]
        return got_here, total

    def reduce_rest(total, axis):
        step = 2
        while counts[axis] > 4 and step < counts[axis]:
            swaps = [(i, i ^ step) for i in range(counts[axis])]
            total = total + lax.ppermute(total, axis, swaps)
            step *= 2
        return total

    total = sums
    gx_a, total = stage(fx_a, total, "gx", False, True)
    wide = counts["gx"] == 4
    gx_b, total = stage(jnp.concatenate([fx_b, total]), total, "gx", True, wide)
    total = reduce_rest(total, "gx")
    gy_a, total = stage(jnp.concatenate([fy[0], total]), total, "gy", False, True)
    gy = [gy_a]
    if two_y:
        wide = counts["gy"] == 4
        gy_b, total = stage(jnp.concatenate([fy[1], total]), total, "gy", True, wide)
        gy.append(gy_b)
        total = reduce_rest(total, "gy")

    def z_payload(face):
        return jnp.concatenate([face, jnp.concatenate([total[:8], total[8:]], axis=1)], axis=1)

    def z_total(value):
        return jnp.concatenate([value[:, flat : flat + nz], value[:, flat + nz :]], axis=0)

    gz_a = swap(z_payload(fz_a), "gz")
    total = total + z_total(gz_a)
    gz_b = swap(z_payload(fz_b), "gz", True)
    if counts["gz"] == 4:
        total = total + z_total(gz_b)
    total = reduce_rest(total, "gz")

    block = pl.BlockSpec((1, nx, ny, nz), lambda i: (2, 0, 0, 0))

    def whole(value):
        return pl.BlockSpec(value.shape, lambda i: (0,) * value.ndim)

    rest = [div, slope, total, gx_a, gx_b, *gy, gz_a, gz_b]
    vel_new, source, forcing_new = pl.pallas_call(
        optional(functools.partial(finish_kernel, cells), () if two_y else (9,)),
        grid=(1,),
        out_shape=[f32(3, nx, ny, nz), f32(nx, ny, nz), f32(1)],
        in_specs=[smem, smem, block] + [whole(v) for v in rest],
        out_specs=[block, pl.BlockSpec((nx, ny, nz), lambda i: (0, 0, 0)), smem],
        input_output_aliases={2: 0},
        scratch_shapes=[pltpu.VMEM((flat, nz), jnp.float32)],
        compiler_params=PARAMS,
        name="finish",
    )(forcing, target_flux, ustar, *rest)
    return vel_new, source, forcing_new


def solution(mesh):
    return jax.shard_map(
        local,
        mesh=mesh,
        in_specs=(
            P(None, "gx", "gy", "gz"),
            P("gx", "gy", "gz"),
            P("gx", "gy", "gz"),
            P(None, "gx", "gy", "gz"),
            P(),
            P(),
        ),
        out_specs=(P(None, "gx", "gy", "gz"), P("gx", "gy", "gz"), P()),
        check_vma=False,
    )
```

```python
import functools
import math

import jax
import jax.numpy as jnp
from jax import lax
from jax.experimental import pallas as pl
from jax.experimental.pallas import tpu as pltpu
from jax.sharding import PartitionSpec as P

time_step = 0.2
viscosity = 0.1
drag_scale = 1.0

PARAMS = pltpu.CompilerParams(vmem_limit_bytes=16 * 2**20)


def pairs_a(count):
    return [(i, i ^ 1) for i in range(count)]


def pairs_b(count):
    swaps = []
    for i in range(1, count, 2):
        swaps += [(i, (i + 1) % count), ((i + 1) % count, i)]
    return swaps


def even(axis):
    return lax.axis_index(axis) % 2 == 0


def z_rows(field):
    return field.T


def pack_kernel(
    vel_hbm, pres_hbm, void_hbm, x_a, x_b, y_a, y_b, z_a, z_b, vel, pres, void, columns, sems
):
    copies = [
        pltpu.make_async_copy(src, dst, sems.at[k])
        for k, (src, dst) in enumerate(((vel_hbm, vel), (pres_hbm, pres), (void_hbm, void)))
    ]
    for copy in copies:
        copy.start()
    for copy in copies:
        copy.wait()
    _, nx, ny, nz = vel.shape
    x_even, y_even, z_even = even("gx"), even("gy"), even("gz")
    for out, at in ((x_a, jnp.where(x_even, nx - 1, 0)), (x_b, jnp.where(x_even, 0, nx - 1))):
        for c in range(3):
            out[c] = vel[c, at]
        out[3] = pres[at]
    at_a, at_b = jnp.where(y_even, ny - 1, 0), jnp.where(y_even, 0, ny - 1)
    lane = lax.broadcasted_iota(jnp.int32, (ny, nz), 1)

    def slab(i, carry):
        for out, at in ((y_a, at_a), (y_b, at_b)):
            if out is not None:
                for c in range(3):
                    out[c, pl.ds(i, 1), :] = vel[c, i, pl.ds(at, 1), :]
                out[3, pl.ds(i, 1), :] = pres[i, pl.ds(at, 1), :]
        fields = [vel[0, i], vel[1, i], vel[2, i], pres[i], void[i]]
        joined = pltpu.roll(fields[0], 1, 1)
        for f in range(1, 5):
            joined = jnp.where(lane >= 2 * f, pltpu.roll(fields[f], 2 * f + 1, 1), joined)
        columns[pl.ds(pl.multiple_of(i * ny, ny), ny), :] = joined
        return carry

    lax.fori_loop(0, nx, slab, 0, unroll=4)
    rows = z_rows(columns[...])
    for f in range(5):
        high, low = rows[2 * f : 2 * f + 1], rows[2 * f + 1 : 2 * f + 2]
        z_a[f : f + 1, :] = jnp.where(z_even, high, low)
        z_b[f : f + 1, :] = jnp.where(z_even, low, high)
    for out in (z_a, z_b):
        out[5:8, :] = jnp.zeros((3, out.shape[1]), jnp.float32)


def drag_kernel(vel, void, part, rate, scale, void_part):
    _, nx, ny, nz = vel.shape

    def slab(i, acc):
        eps = void[i]
        slip2 = sum((vel[c, i] - part[c, i]) ** 2 for c in range(3))
        here = drag_scale * (1.0 - eps) * jnp.exp(-2.65 * jnp.log(eps)) * (1.0 + jnp.sqrt(slip2))
        rate[i] = time_step * here
        scale[i] = 1.0 / (1.0 + time_step * here)
        return acc + eps

    acc = lax.fori_loop(0, nx, slab, jnp.zeros((ny, nz), jnp.float32), unroll=4)
    void_part[...] = fold(acc)


def fold(value):
    return functools.reduce(jnp.add, [value[8 * k : 8 * k + 8] for k in range(value.shape[0] // 8)])


class Stencil:
    def __init__(self, vel, pres, halo, x_a, x_b, y_a, y_b):
        _, self.nx, self.ny, self.nz = vel.shape
        self.vel, self.pres, self.halo = vel, pres, halo
        self.x, self.y = (x_a, x_b), (y_a, y_b)
        self.x_even, self.y_even = even("gx"), even("gy")
        xi, yi = lax.axis_index("gx"), lax.axis_index("gy")
        self.x_low, self.x_high = xi == 0, xi == lax.axis_size("gx") - 1
        self.y_low, self.y_high = yi == 0, yi == lax.axis_size("gy") - 1
        self.lane = lax.broadcasted_iota(jnp.int32, (self.ny, self.nz), 1)
        self.row = lax.broadcasted_iota(jnp.int32, (self.ny, self.nz), 0)

    def load(self, f, i):
        return self.vel[f, i] if f < 3 else self.pres[i]

    def along_x(self, f, i, first, last):
        a, b = self.x
        if first:
            wall = 0.0 if f < 3 else self.pres[0]
            low = jnp.where(self.x_low, wall, jnp.where(self.x_even, b[f], a[f]))
        else:
            low = self.load(f, i - 1)
        if last:
            wall = 0.0 if f < 3 else self.pres[self.nx - 1]
            high = jnp.where(self.x_high, wall, jnp.where(self.x_even, a[f], b[f]))
        else:
            high = self.load(f, i + 1)
        return low, high

    def along_y(self, f, i):
        here = self.load(f, i)
        row_a = self.y[0][f, pl.ds(i, 1), :]
        row_b = self.y[1][f, pl.ds(i, 1), :] if self.y[1] is not None else row_a
        wall_low = 0.0 if f < 3 else here[0:1]
        wall_high = 0.0 if f < 3 else here[self.ny - 1 : self.ny]
        low = jnp.where(self.y_low, wall_low, jnp.where(self.y_even, row_b, row_a))
        high = jnp.where(self.y_high, wall_high, jnp.where(self.y_even, row_a, row_b))
        return (
            jnp.where(self.row == 0, low, pltpu.roll(here, 1, 0)),
            jnp.where(self.row == self.ny - 1, high, pltpu.roll(here, self.ny - 1, 0)),
        )

    def rows_at(self, i):
        return pl.ds(i * self.ny if isinstance(i, int) else pl.multiple_of(i * self.ny, self.ny), self.ny)

    def along_z(self, here, f, i):
        edge = self.halo[self.rows_at(i), :]
        low = jnp.where(self.lane == 0, edge[:, f : f + 1], pltpu.roll(here, 1, 1))
        high = jnp.where(
            self.lane == self.nz - 1, edge[:, 8 + f : 9 + f], pltpu.roll(here, self.nz - 1, 1)
        )
        return low, high

    def ustar(self, c, i, first, last, part, rate, scale, push):
        here = self.load(c, i)
        xm, xp = self.along_x(c, i, first, last)
        ym, yp = self.along_y(c, i)
        zm, zp = self.along_z(here, c, i)
        u = [self.load(d, i) for d in range(3)]
        advection = (u[0] * (xp - xm) + u[1] * (yp - ym) + u[2] * (zp - zm)) * 0.5
        laplace = (xm + xp) + (ym + yp) + (zm + zp) - 6.0 * here
        if c == 0:
            pm, pp = self.along_x(3, i, first, last)
        elif c == 1:
            pm, pp = self.along_y(3, i)
        else:
            pm, pp = self.along_z(self.load(3, i), 3, i)
        force = viscosity * laplace - advection - (pp - pm) * 0.5
        if push is not None:
            force = force + push
        return (here + time_step * force + rate[i] * part[i]) * scale[i]


def sweep(nx, slab, acc, unroll=4):
    acc = slab(0, True, False, acc)
    inner = (nx - 2) // unroll * unroll
    acc = lax.fori_loop(1, 1 + inner, lambda i, a: slab(i, False, False, a), acc, unroll=unroll)
    for i in range(1 + inner, nx - 1):
        acc = slab(i, False, False, acc)
    return slab(nx - 1, False, True, acc)


def z_kernel(
    forcing, vel, pres, void, part, rate, scale, void_part, x_a, x_b, y_a, y_b, z_a, z_b,
    uz, flux, slope, fz_a, fz_b, sums, halo,
):
    _, nx, ny, nz = vel.shape
    z_even = even("gz")
    low_rows = jnp.where(z_even, z_b[...], z_a[...])
    high_rows = jnp.where(z_even, z_a[...], z_b[...])
    halo[...] = jnp.concatenate(
        [low_rows, high_rows, jnp.zeros((nz - 16, low_rows.shape[1]), jnp.float32)], axis=0
    ).T
    near = Stencil(vel, pres, halo, x_a, x_b, y_a, y_b)
    push = forcing[0]

    def slab(i, first, last, acc):
        value = near.ustar(2, i, first, last, part.at[0], rate, scale, push)
        uz[i] = value
        eps = void[i]
        em, ep = near.along_z(eps, 4, i)
        slope[i] = (ep - em) * 0.5
        flow = eps * value
        flux[near.rows_at(i), :] = flow
        return acc + flow

    acc = sweep(nx, slab, jnp.zeros((ny, nz), jnp.float32))
    sums[0:8] = fold(acc)
    sums[8:16] = void_part[...]
    turned = z_rows(flux[...])
    z_low, z_high = turned[0:1], turned[nz - 1 : nz]
    send_a, send_b = jnp.where(z_even, z_high, z_low), jnp.where(z_even, z_low, z_high)
    width = turned.shape[1]
    for out, send in ((fz_a, send_a), (fz_b, send_b)):
        out[:, 0:width] = jnp.broadcast_to(send, (8, width))
    fz_a[:, width : width + nz] = sums[0:8]
    fz_a[:, width + nz : width + 2 * nz] = sums[8:16]


def y_kernel(
    vel, pres, void, part, rate, scale, flux_z, halo, x_a, x_b, y_a, y_b,
    out, div, fy_a, fy_b,
):
    _, nx, ny, nz = vel.shape
    near = Stencil(vel, pres, halo, x_a, x_b, y_a, y_b)

    def slab(i, first, last, acc):
        value = near.ustar(1, i, first, last, part.at[0], rate, scale, None)
        out[0, i] = value
        flow = void[i] * value
        ym = jnp.where(near.row == 0, 0.0, pltpu.roll(flow, 1, 0))
        yp = jnp.where(near.row == ny - 1, 0.0, pltpu.roll(flow, ny - 1, 0))
        up = flux_z[near.rows_at(i), :]
        zm = jnp.where(near.lane == 0, 0.0, pltpu.roll(up, 1, 1))
        zp = jnp.where(near.lane == nz - 1, 0.0, pltpu.roll(up, nz - 1, 1))
        div[i] = ((yp - ym) + (zp - zm)) * 0.5
        first_row, last_row = flow[0:1], flow[ny - 1 : ny]
        fy_a[pl.ds(i, 1), :] = jnp.where(near.y_even, last_row, first_row)
        if fy_b is not None:
            fy_b[pl.ds(i, 1), :] = jnp.where(near.y_even, first_row, last_row)
        return acc

    sweep(nx, slab, 0)


def x_kernel(
    kept, vel, pres, void, part, rate, scale, halo, div_yz, x_a, x_b, y_a, y_b,
    out, div, fx_a, fx_b, flux,
):
    _, nx, ny, nz = vel.shape
    near = Stencil(vel, pres, halo, x_a, x_b, y_a, y_b)

    def slab(i, first, last, acc):
        value = near.ustar(0, i, first, last, part.at[0], rate, scale, None)
        out[0, i] = value
        flux[i] = void[i] * value
        return acc

    sweep(nx, slab, 0)

    def join(i, first, last, acc):
        low = 0.0 if first else flux[i - 1]
        high = 0.0 if last else flux[i + 1]
        div[i] = div_yz[i] + (high - low) * 0.5
        return acc

    sweep(nx, join, 0)
    low, high = flux[0], flux[nx - 1]
    fx_a[...] = jnp.where(near.x_even, high, low)
    fx_b[...] = jnp.where(near.x_even, low, high)


def edge_kernel(div, fy_a, fy_b, fz_a, fz_b, out, halo):
    nx, ny, nz = div.shape
    y_even, z_even = even("gy"), even("gz")
    yi = lax.axis_index("gy")
    y_low, y_high = yi == 0, yi == lax.axis_size("gy") - 1
    a, b = fz_a[0:1, 0 : nx * ny], fz_b[0:1, 0 : nx * ny]
    low_row, high_row = jnp.where(z_even, b, a), jnp.where(z_even, a, b)
    pick = lax.broadcasted_iota(jnp.int32, (nz, halo.shape[0]), 0)
    halo[...] = jnp.where(pick == 0, -low_row, jnp.where(pick == nz - 1, high_row, 0.0)).T
    row = lax.broadcasted_iota(jnp.int32, (ny, nz), 0)

    def slab(i, carry):
        rows_at = pl.ds(pl.multiple_of(i * ny, ny), ny)
        row_a = fy_a[pl.ds(i, 1), :]
        row_b = fy_b[pl.ds(i, 1), :] if fy_b is not None else row_a
        ym = jnp.where(y_low, 0.0, jnp.where(y_even, row_b, row_a))
        yp = jnp.where(y_high, 0.0, jnp.where(y_even, row_a, row_b))
        ends = jnp.where(row == 0, -ym, jnp.where(row == ny - 1, yp, 0.0)) + halo[rows_at, :]
        out[i] = div[i] + 0.5 * ends
        return carry

    lax.fori_loop(0, nx, slab, 0, unroll=4)


def finish_kernel(
    cells, forcing, target, kept, uz, div, slope, sums, fx_a, fx_b, vel_new, source, forcing_new
):
    nx, ny, nz = div.shape
    x_even = even("gx")
    xi = lax.axis_index("gx")
    x_low, x_high = xi == 0, xi == lax.axis_size("gx") - 1
    flow, total = jnp.sum(sums[0:8]), jnp.sum(sums[8:16])
    step = (target[0] * cells - flow) / (time_step * total)
    forcing_new[0] = forcing[0] + step
    rise = time_step * step
    xl = jnp.where(x_low, 0.0, jnp.where(x_even, fx_b[0:ny], fx_a[0:ny]))
    xh = jnp.where(x_high, 0.0, jnp.where(x_even, fx_a[0:ny], fx_b[0:ny]))

    def slab(i, first, last, acc):
        value = div[i] + rise * slope[i]
        if first:
            value = value - 0.5 * xl
        if last:
            value = value + 0.5 * xh
        source[i] = value
        vel_new[0, i] = uz[i] + rise
        return acc

    sweep(nx, slab, 0)


def swap(value, axis, second=False):
    count = lax.axis_size(axis)
    return lax.ppermute(value, axis, pairs_b(count) if second else pairs_a(count))


def optional(kernel, slots):
    def run(*refs):
        refs = list(refs)
        for slot in slots:
            refs.insert(slot, None)
        return kernel(*refs)

    return run


def f32(*shape):
    return jax.ShapeDtypeStruct(shape, jnp.float32)


def local(velocity, pressure, voidage, particle_vel, forcing, target_flux):
    _, nx, ny, nz = velocity.shape
    counts = {axis: lax.axis_size(axis) for axis in ("gx", "gy", "gz")}
    cells = float(voidage.size * math.prod(counts.values()))
    two_y = counts["gy"] > 2
    flat = nx * ny
    smem = pl.BlockSpec(memory_space=pltpu.SMEM)
    vmem = pl.BlockSpec(memory_space=pltpu.VMEM)

    any_space = pl.BlockSpec(memory_space=pl.ANY)
    y_out = [f32(4, nx, nz)] * (2 if two_y else 1)
    faces = pl.pallas_call(
        optional(pack_kernel, () if two_y else (6,)),
        out_shape=[f32(4, ny, nz), f32(4, ny, nz)] + y_out + [f32(8, flat)] * 2
        + [f32(*v.shape) for v in (velocity, pressure, voidage)],
        in_specs=[pl.BlockSpec(memory_space=pltpu.HBM)] * 3,
        scratch_shapes=[pltpu.VMEM((flat, nz), jnp.float32), pltpu.SemaphoreType.DMA((3,))],
        compiler_params=PARAMS,
        name="pack",
    )(velocity, pressure, voidage)
    x_a, x_b, *y_faces, z_a, z_b, velocity, pressure, voidage = faces
    near = [swap(x_a, "gx"), swap(x_b, "gx", True)]
    near += [swap(y, "gy", k == 1) for k, y in enumerate(y_faces)]
    z_near = [swap(z_a, "gz"), swap(z_b, "gz", True)]

    cube = f32(nx, ny, nz)
    rate, scale, void_part = pl.pallas_call(
        drag_kernel,
        out_shape=[cube, cube, f32(8, nz)],
        in_specs=[vmem] * 3,
        compiler_params=PARAMS,
        name="drag",
    )(velocity, voidage, particle_vel)

    def whole(value):
        return pl.BlockSpec(value.shape, lambda i: (0,) * len(value.shape))

    def one(c):
        return pl.BlockSpec((1, nx, ny, nz), lambda i: (c, 0, 0, 0))

    def call(kernel, args, specs, outs, out_specs, name, **more):
        return pl.pallas_call(
            kernel,
            grid=(1,),
            in_specs=[whole(v) if spec is None else spec for v, spec in zip(args, specs)],
            out_shape=outs,
            out_specs=[whole(v) if spec is None else spec for v, spec in zip(outs, out_specs)],
            compiler_params=PARAMS,
            name=name,
            **more,
        )(*args)

    args = [forcing, velocity, pressure, voidage, particle_vel, rate, scale, void_part, *near, *z_near]
    outs = [cube, f32(flat, nz), cube, f32(8, flat + 2 * nz), f32(8, flat), f32(16, nz), f32(flat, nz)]
    uz, flux_z, slope, fz_a, fz_b, sums, halo = call(
        optional(z_kernel, () if two_y else (11,)),
        args, [smem, None, None, None, one(2)] + [None] * (len(args) - 5), outs, [None] * len(outs), "z",
    )
    gz_a = swap(fz_a, "gz")

    args = [velocity, pressure, voidage, particle_vel, rate, scale, flux_z, halo, *near]
    outs = [f32(3, nx, ny, nz), cube] + [f32(nx, nz)] * len(y_faces)
    vel_y, div_yz, *fy = call(
        optional(y_kernel, () if two_y else (11, 15)),
        args, [None, None, None, one(1)] + [None] * (len(args) - 4),
        outs, [one(1)] + [None] * (len(outs) - 1), "y",
    )
    fz_b, fy[0] = lax.optimization_barrier((fz_b, fy[0]))

    def z_total(value):
        return jnp.concatenate([value[:, flat : flat + nz], value[:, flat + nz :]], axis=0)

    def reduce_rest(total, axis):
        step = 2
        while counts[axis] > 4 and step < counts[axis]:
            swaps = [(i, i ^ step) for i in range(counts[axis])]
            total = total + lax.ppermute(total, axis, swaps)
            step *= 2
        return total

    def second(face, total, axis):
        got = swap(jnp.concatenate([face, total]), axis, True)
        if counts[axis] == 4:
            total = total + got[-16:]
        return got, reduce_rest(total, axis)

    total = sums + z_total(gz_a)
    gz_b = swap(jnp.concatenate([fz_b, total[:8], total[8:]], axis=1), "gz", True)

    args = [vel_y, velocity, pressure, voidage, particle_vel, rate, scale, halo, div_yz, *near]
    outs = [f32(3, nx, ny, nz), cube, f32(ny, nz), f32(ny, nz)]
    vel_xy, div, fx_a, fx_b = call(
        optional(x_kernel, () if two_y else (12,)),
        args, [any_space, None, None, None, one(0)] + [None] * (len(args) - 5),
        outs, [one(0)] + [None] * 3, "x",
        input_output_aliases={0: 0},
        scratch_shapes=[pltpu.VMEM((nx, ny, nz), jnp.float32)],
    )
    if counts["gz"] == 4:
        total = total + z_total(gz_b)
    total = reduce_rest(total, "gz")

    face, fx_a, fx_b = lax.optimization_barrier((fy[0], fx_a, fx_b))
    gy = [swap(jnp.concatenate([face, total]), "gy")]
    total = total + gy[0][-16:]
    if two_y:
        got, total = second(fy[1], total, "gy")
        gy.append(got)

    gx_a = swap(jnp.concatenate([fx_a, total]), "gx")
    total = total + gx_a[-16:]
    args = [div, *gy, gz_a, gz_b]
    (div,) = call(
        optional(edge_kernel, () if two_y else (2,)),
        args, [None] * len(args), [cube], [None], "edge",
        scratch_shapes=[pltpu.VMEM((flat, nz), jnp.float32)],
    )
    fx_b, div = lax.optimization_barrier((fx_b, div))
    gx_b, total = second(fx_b, total, "gx")

    args = [forcing, target_flux, vel_xy, uz, div, slope, total, gx_a, gx_b]
    vel_new, source, forcing_new = call(
        functools.partial(finish_kernel, cells),
        args, [smem, smem, any_space] + [None] * (len(args) - 3),
        [f32(3, nx, ny, nz), cube, f32(1)], [one(2), None, smem], "finish",
        input_output_aliases={2: 0},
    )
    return vel_new, source, forcing_new


def solution(mesh):
    return jax.shard_map(
        local,
        mesh=mesh,
        in_specs=(
            P(None, "gx", "gy", "gz"),
            P("gx", "gy", "gz"),
            P("gx", "gy", "gz"),
            P(None, "gx", "gy", "gz"),
            P(),
            P(),
        ),
        out_specs=(P(None, "gx", "gy", "gz"), P("gx", "gy", "gz"), P()),
        check_vma=False,
    )
```

```python
import functools
import math

import jax
import jax.numpy as jnp
from jax import lax
from jax.experimental import pallas as pl
from jax.experimental.pallas import tpu as pltpu
from jax.sharding import PartitionSpec as P

time_step = 0.2
viscosity = 0.1
drag_scale = 1.0

PARAMS = pltpu.CompilerParams(vmem_limit_bytes=16 * 2**20)


def pairs_a(count):
    return [(i, i ^ 1) for i in range(count)]


def pairs_b(count):
    swaps = []
    for i in range(1, count, 2):
        swaps += [(i, (i + 1) % count), ((i + 1) % count, i)]
    return swaps


def even(axis):
    return lax.axis_index(axis) % 2 == 0


def z_rows(field):
    return field.T


def pack_kernel(
    vel_hbm, pres_hbm, void_hbm, x_a, x_b, y_a, y_b, z_a, z_b, columns, vel, pres, void, sems
):
    copies = [
        pltpu.make_async_copy(src, dst, sems.at[k])
        for k, (src, dst) in enumerate(((vel_hbm, vel), (pres_hbm, pres), (void_hbm, void)))
    ]
    for copy in copies:
        copy.start()
    for copy in copies:
        copy.wait()
    _, nx, ny, nz = vel.shape
    x_even, y_even, z_even = even("gx"), even("gy"), even("gz")
    for out, at in ((x_a, jnp.where(x_even, nx - 1, 0)), (x_b, jnp.where(x_even, 0, nx - 1))):
        for c in range(3):
            out[c] = vel[c, at]
        out[3] = pres[at]
    at_a, at_b = jnp.where(y_even, ny - 1, 0), jnp.where(y_even, 0, ny - 1)
    lane = lax.broadcasted_iota(jnp.int32, (ny, nz), 1)

    def slab(i, carry):
        for out, at in ((y_a, at_a), (y_b, at_b)):
            if out is not None:
                for c in range(3):
                    out[c, pl.ds(i, 1), :] = vel[c, i, pl.ds(at, 1), :]
                out[3, pl.ds(i, 1), :] = pres[i, pl.ds(at, 1), :]
        fields = [vel[0, i], vel[1, i], vel[2, i], pres[i], void[i]]
        joined = pltpu.roll(fields[0], 1, 1)
        for f in range(1, 5):
            joined = jnp.where(lane >= 2 * f, pltpu.roll(fields[f], 2 * f + 1, 1), joined)
        columns[pl.ds(pl.multiple_of(i * ny, ny), ny), :] = joined
        return carry

    lax.fori_loop(0, nx, slab, 0, unroll=4)
    rows = z_rows(columns[...])
    for f in range(5):
        high, low = rows[2 * f : 2 * f + 1], rows[2 * f + 1 : 2 * f + 2]
        z_a[f : f + 1, :] = jnp.where(z_even, high, low)
        z_b[f : f + 1, :] = jnp.where(z_even, low, high)
    for out in (z_a, z_b):
        out[5:8, :] = jnp.zeros((3, out.shape[1]), jnp.float32)


def drag_kernel(vel, void, part, rate, scale, void_part):
    _, nx, ny, nz = vel.shape

    def slab(i, acc):
        eps = void[i]
        slip2 = sum((vel[c, i] - part[c, i]) ** 2 for c in range(3))
        here = drag_scale * (1.0 - eps) * jnp.exp(-2.65 * jnp.log(eps)) * (1.0 + jnp.sqrt(slip2))
        rate[i] = time_step * here
        scale[i] = 1.0 / (1.0 + time_step * here)
        return acc + eps

    acc = lax.fori_loop(0, nx, slab, jnp.zeros((ny, nz), jnp.float32), unroll=4)
    void_part[...] = fold(acc)


def fold(value):
    return functools.reduce(jnp.add, [value[8 * k : 8 * k + 8] for k in range(value.shape[0] // 8)])


class Stencil:
    def __init__(self, vel, pres, halo, x_a, x_b, y_a, y_b):
        _, self.nx, self.ny, self.nz = vel.shape
        self.vel, self.pres, self.halo = vel, pres, halo
        self.x, self.y = (x_a, x_b), (y_a, y_b)
        self.x_even, self.y_even = even("gx"), even("gy")
        xi, yi = lax.axis_index("gx"), lax.axis_index("gy")
        self.x_low, self.x_high = xi == 0, xi == lax.axis_size("gx") - 1
        self.y_low, self.y_high = yi == 0, yi == lax.axis_size("gy") - 1
        self.lane = lax.broadcasted_iota(jnp.int32, (self.ny, self.nz), 1)
        self.row = lax.broadcasted_iota(jnp.int32, (self.ny, self.nz), 0)

    def load(self, f, i):
        return self.vel[f, i] if f < 3 else self.pres[i]

    def along_x(self, f, i, first, last):
        a, b = self.x
        if first:
            wall = 0.0 if f < 3 else self.pres[0]
            low = jnp.where(self.x_low, wall, jnp.where(self.x_even, b[f], a[f]))
        else:
            low = self.load(f, i - 1)
        if last:
            wall = 0.0 if f < 3 else self.pres[self.nx - 1]
            high = jnp.where(self.x_high, wall, jnp.where(self.x_even, a[f], b[f]))
        else:
            high = self.load(f, i + 1)
        return low, high

    def along_y(self, f, i):
        here = self.load(f, i)
        row_a = self.y[0][f, pl.ds(i, 1), :]
        row_b = self.y[1][f, pl.ds(i, 1), :] if self.y[1] is not None else row_a
        wall_low = 0.0 if f < 3 else here[0:1]
        wall_high = 0.0 if f < 3 else here[self.ny - 1 : self.ny]
        low = jnp.where(self.y_low, wall_low, jnp.where(self.y_even, row_b, row_a))
        high = jnp.where(self.y_high, wall_high, jnp.where(self.y_even, row_a, row_b))
        return (
            jnp.where(self.row == 0, low, pltpu.roll(here, 1, 0)),
            jnp.where(self.row == self.ny - 1, high, pltpu.roll(here, self.ny - 1, 0)),
        )

    def rows_at(self, i):
        return pl.ds(i * self.ny if isinstance(i, int) else pl.multiple_of(i * self.ny, self.ny), self.ny)

    def along_z(self, here, f, i):
        edge = self.halo[self.rows_at(i), :]
        low = jnp.where(self.lane == 0, edge[:, f : f + 1], pltpu.roll(here, 1, 1))
        high = jnp.where(
            self.lane == self.nz - 1, edge[:, 8 + f : 9 + f], pltpu.roll(here, self.nz - 1, 1)
        )
        return low, high

    def ustar(self, c, i, first, last, part, rate, scale, push):
        here = self.load(c, i)
        xm, xp = self.along_x(c, i, first, last)
        ym, yp = self.along_y(c, i)
        zm, zp = self.along_z(here, c, i)
        u = [self.load(d, i) for d in range(3)]
        advection = (u[0] * (xp - xm) + u[1] * (yp - ym) + u[2] * (zp - zm)) * 0.5
        laplace = (xm + xp) + (ym + yp) + (zm + zp) - 6.0 * here
        if c == 0:
            pm, pp = self.along_x(3, i, first, last)
        elif c == 1:
            pm, pp = self.along_y(3, i)
        else:
            pm, pp = self.along_z(self.load(3, i), 3, i)
        force = viscosity * laplace - advection - (pp - pm) * 0.5
        if push is not None:
            force = force + push
        return (here + time_step * force + rate[i] * part[i]) * scale[i]


def sweep(nx, slab, acc, unroll=4):
    acc = slab(0, True, False, acc)
    inner = (nx - 2) // unroll * unroll
    acc = lax.fori_loop(1, 1 + inner, lambda i, a: slab(i, False, False, a), acc, unroll=unroll)
    for i in range(1 + inner, nx - 1):
        acc = slab(i, False, False, acc)
    return slab(nx - 1, False, True, acc)


def z_kernel(
    forcing, vel, pres, void, part, rate, scale, void_part, x_a, x_b, y_a, y_b, z_a, z_b,
    uz, flux, slope, fz_a, fz_b, sums, halo,
):
    _, nx, ny, nz = vel.shape
    z_even = even("gz")
    low_rows = jnp.where(z_even, z_b[...], z_a[...])
    high_rows = jnp.where(z_even, z_a[...], z_b[...])
    halo[...] = jnp.concatenate(
        [low_rows, high_rows, jnp.zeros((nz - 16, low_rows.shape[1]), jnp.float32)], axis=0
    ).T
    near = Stencil(vel, pres, halo, x_a, x_b, y_a, y_b)
    push = forcing[0]

    def slab(i, first, last, acc):
        value = near.ustar(2, i, first, last, part.at[0], rate, scale, push)
        uz[i] = value
        eps = void[i]
        em, ep = near.along_z(eps, 4, i)
        slope[i] = (ep - em) * 0.5
        flow = eps * value
        flux[near.rows_at(i), :] = flow
        return acc + flow

    acc = sweep(nx, slab, jnp.zeros((ny, nz), jnp.float32))
    sums[0:8] = fold(acc)
    sums[8:16] = void_part[...]
    turned = z_rows(flux[...])
    z_low, z_high = turned[0:1], turned[nz - 1 : nz]
    send_a, send_b = jnp.where(z_even, z_high, z_low), jnp.where(z_even, z_low, z_high)
    width = turned.shape[1]
    for out, send in ((fz_a, send_a), (fz_b, send_b)):
        out[:, 0:width] = jnp.broadcast_to(send, (8, width))
    fz_a[:, width : width + nz] = sums[0:8]
    fz_a[:, width + nz : width + 2 * nz] = sums[8:16]


def y_kernel(
    vel, pres, void, part, rate, scale, flux_z, halo, x_a, x_b, y_a, y_b,
    out, div, fy_a, fy_b,
):
    _, nx, ny, nz = vel.shape
    near = Stencil(vel, pres, halo, x_a, x_b, y_a, y_b)

    def slab(i, first, last, acc):
        value = near.ustar(1, i, first, last, part.at[0], rate, scale, None)
        out[0, i] = value
        flow = void[i] * value
        ym = jnp.where(near.row == 0, 0.0, pltpu.roll(flow, 1, 0))
        yp = jnp.where(near.row == ny - 1, 0.0, pltpu.roll(flow, ny - 1, 0))
        up = flux_z[near.rows_at(i), :]
        zm = jnp.where(near.lane == 0, 0.0, pltpu.roll(up, 1, 1))
        zp = jnp.where(near.lane == nz - 1, 0.0, pltpu.roll(up, nz - 1, 1))
        div[i] = ((yp - ym) + (zp - zm)) * 0.5
        first_row, last_row = flow[0:1], flow[ny - 1 : ny]
        fy_a[pl.ds(i, 1), :] = jnp.where(near.y_even, last_row, first_row)
        if fy_b is not None:
            fy_b[pl.ds(i, 1), :] = jnp.where(near.y_even, first_row, last_row)
        return acc

    sweep(nx, slab, 0)


def x_kernel(
    kept, vel, pres, void, part, rate, scale, halo, div_yz, x_a, x_b, y_a, y_b,
    out, div, fx_a, fx_b, flux,
):
    _, nx, ny, nz = vel.shape
    near = Stencil(vel, pres, halo, x_a, x_b, y_a, y_b)

    def slab(i, first, last, acc):
        value = near.ustar(0, i, first, last, part.at[0], rate, scale, None)
        out[0, i] = value
        flux[i] = void[i] * value
        return acc

    sweep(nx, slab, 0)

    def join(i, first, last, acc):
        low = 0.0 if first else flux[i - 1]
        high = 0.0 if last else flux[i + 1]
        div[i] = div_yz[i] + (high - low) * 0.5
        return acc

    sweep(nx, join, 0)
    low, high = flux[0], flux[nx - 1]
    fx_a[...] = jnp.where(near.x_even, high, low)
    fx_b[...] = jnp.where(near.x_even, low, high)


def edge_kernel(div, fy_a, fy_b, fz_a, fz_b, out, halo):
    nx, ny, nz = div.shape
    y_even, z_even = even("gy"), even("gz")
    yi = lax.axis_index("gy")
    y_low, y_high = yi == 0, yi == lax.axis_size("gy") - 1
    a, b = fz_a[0:1, 0 : nx * ny], fz_b[0:1, 0 : nx * ny]
    low_row, high_row = jnp.where(z_even, b, a), jnp.where(z_even, a, b)
    pick = lax.broadcasted_iota(jnp.int32, (nz, halo.shape[0]), 0)
    halo[...] = jnp.where(pick == 0, -low_row, jnp.where(pick == nz - 1, high_row, 0.0)).T
    row = lax.broadcasted_iota(jnp.int32, (ny, nz), 0)

    def slab(i, carry):
        rows_at = pl.ds(pl.multiple_of(i * ny, ny), ny)
        row_a = fy_a[pl.ds(i, 1), :]
        row_b = fy_b[pl.ds(i, 1), :] if fy_b is not None else row_a
        ym = jnp.where(y_low, 0.0, jnp.where(y_even, row_b, row_a))
        yp = jnp.where(y_high, 0.0, jnp.where(y_even, row_a, row_b))
        ends = jnp.where(row == 0, -ym, jnp.where(row == ny - 1, yp, 0.0)) + halo[rows_at, :]
        out[i] = div[i] + 0.5 * ends
        return carry

    lax.fori_loop(0, nx, slab, 0, unroll=4)


def finish_kernel(
    cells, forcing, target, kept, uz, div, slope, sums, fx_a, fx_b, vel_new, source, forcing_new
):
    nx, ny, nz = div.shape
    x_even = even("gx")
    xi = lax.axis_index("gx")
    x_low, x_high = xi == 0, xi == lax.axis_size("gx") - 1
    flow, total = jnp.sum(sums[0:8]), jnp.sum(sums[8:16])
    step = (target[0] * cells - flow) / (time_step * total)
    forcing_new[0] = forcing[0] + step
    rise = time_step * step
    xl = jnp.where(x_low, 0.0, jnp.where(x_even, fx_b[0:ny], fx_a[0:ny]))
    xh = jnp.where(x_high, 0.0, jnp.where(x_even, fx_a[0:ny], fx_b[0:ny]))

    def slab(i, first, last, acc):
        value = div[i] + rise * slope[i]
        if first:
            value = value - 0.5 * xl
        if last:
            value = value + 0.5 * xh
        source[i] = value
        vel_new[0, i] = uz[i] + rise
        return acc

    sweep(nx, slab, 0)


def swap(value, axis, second=False):
    count = lax.axis_size(axis)
    return lax.ppermute(value, axis, pairs_b(count) if second else pairs_a(count))


def optional(kernel, slots):
    def run(*refs):
        refs = list(refs)
        for slot in slots:
            refs.insert(slot, None)
        return kernel(*refs)

    return run


def f32(*shape):
    return jax.ShapeDtypeStruct(shape, jnp.float32)


def local(velocity, pressure, voidage, particle_vel, forcing, target_flux):
    _, nx, ny, nz = velocity.shape
    counts = {axis: lax.axis_size(axis) for axis in ("gx", "gy", "gz")}
    cells = float(voidage.size * math.prod(counts.values()))
    two_y = counts["gy"] > 2
    flat = nx * ny
    smem = pl.BlockSpec(memory_space=pltpu.SMEM)
    vmem = pl.BlockSpec(memory_space=pltpu.VMEM)

    any_space = pl.BlockSpec(memory_space=pl.ANY)
    y_out = [f32(4, nx, nz)] * (2 if two_y else 1)
    faces = pl.pallas_call(
        optional(pack_kernel, () if two_y else (6,)),
        out_shape=[f32(4, ny, nz), f32(4, ny, nz)] + y_out + [f32(8, flat)] * 2,
        in_specs=[pl.BlockSpec(memory_space=pltpu.HBM)] * 3,
        scratch_shapes=[pltpu.VMEM((flat, nz), jnp.float32)]
        + [pltpu.VMEM(v.shape, jnp.float32) for v in (velocity, pressure, voidage)]
        + [pltpu.SemaphoreType.DMA((3,))],
        compiler_params=pltpu.CompilerParams(vmem_limit_bytes=61000 * 2**10),
        name="pack",
    )(velocity, pressure, voidage)
    x_a, x_b, *y_faces, z_a, z_b = faces
    near = [swap(x_a, "gx"), swap(x_b, "gx", True)]
    near += [swap(y, "gy", k == 1) for k, y in enumerate(y_faces)]
    z_near = [swap(z_a, "gz"), swap(z_b, "gz", True)]

    cube = f32(nx, ny, nz)
    rate, scale, void_part = pl.pallas_call(
        drag_kernel,
        out_shape=[cube, cube, f32(8, nz)],
        in_specs=[vmem] * 3,
        compiler_params=PARAMS,
        name="drag",
    )(velocity, voidage, particle_vel)

    def whole(value):
        return pl.BlockSpec(value.shape, lambda i: (0,) * len(value.shape))

    def one(c):
        return pl.BlockSpec((1, nx, ny, nz), lambda i: (c, 0, 0, 0))

    def call(kernel, args, specs, outs, out_specs, name, **more):
        return pl.pallas_call(
            kernel,
            grid=(1,),
            in_specs=[whole(v) if spec is None else spec for v, spec in zip(args, specs)],
            out_shape=outs,
            out_specs=[whole(v) if spec is None else spec for v, spec in zip(outs, out_specs)],
            compiler_params=PARAMS,
            name=name,
            **more,
        )(*args)

    args = [forcing, velocity, pressure, voidage, particle_vel, rate, scale, void_part, *near, *z_near]
    outs = [cube, f32(flat, nz), cube, f32(8, flat + 2 * nz), f32(8, flat), f32(16, nz), f32(flat, nz)]
    uz, flux_z, slope, fz_a, fz_b, sums, halo = call(
        optional(z_kernel, () if two_y else (11,)),
        args, [smem, None, None, None, one(2)] + [None] * (len(args) - 5), outs, [None] * len(outs), "z",
    )
    gz_a = swap(fz_a, "gz")

    args = [velocity, pressure, voidage, particle_vel, rate, scale, flux_z, halo, *near]
    outs = [f32(3, nx, ny, nz), cube] + [f32(nx, nz)] * len(y_faces)
    vel_y, div_yz, *fy = call(
        optional(y_kernel, () if two_y else (11, 15)),
        args, [None, None, None, one(1)] + [None] * (len(args) - 4),
        outs, [one(1)] + [None] * (len(outs) - 1), "y",
    )
    fz_b, fy[0] = lax.optimization_barrier((fz_b, fy[0]))

    def z_total(value):
        return jnp.concatenate([value[:, flat : flat + nz], value[:, flat + nz :]], axis=0)

    def reduce_rest(total, axis):
        step = 2
        while counts[axis] > 4 and step < counts[axis]:
            swaps = [(i, i ^ step) for i in range(counts[axis])]
            total = total + lax.ppermute(total, axis, swaps)
            step *= 2
        return total

    def second(face, total, axis):
        got = swap(jnp.concatenate([face, total]), axis, True)
        if counts[axis] == 4:
            total = total + got[-16:]
        return got, reduce_rest(total, axis)

    total = sums + z_total(gz_a)
    gz_b = swap(jnp.concatenate([fz_b, total[:8], total[8:]], axis=1), "gz", True)

    args = [vel_y, velocity, pressure, voidage, particle_vel, rate, scale, halo, div_yz, *near]
    outs = [f32(3, nx, ny, nz), cube, f32(ny, nz), f32(ny, nz)]
    vel_xy, div, fx_a, fx_b = call(
        optional(x_kernel, () if two_y else (12,)),
        args, [any_space, None, None, None, one(0)] + [None] * (len(args) - 5),
        outs, [one(0)] + [None] * 3, "x",
        input_output_aliases={0: 0},
        scratch_shapes=[pltpu.VMEM((nx, ny, nz), jnp.float32)],
    )
    if counts["gz"] == 4:
        total = total + z_total(gz_b)
    total = reduce_rest(total, "gz")

    face, fx_a, fx_b = lax.optimization_barrier((fy[0], fx_a, fx_b))
    gy = [swap(jnp.concatenate([face, total]), "gy")]
    total = total + gy[0][-16:]
    if two_y:
        got, total = second(fy[1], total, "gy")
        gy.append(got)

    gx_a = swap(jnp.concatenate([fx_a, total]), "gx")
    total = total + gx_a[-16:]
    args = [div, *gy, gz_a, gz_b]
    (div,) = call(
        optional(edge_kernel, () if two_y else (2,)),
        args, [None] * len(args), [cube], [None], "edge",
        scratch_shapes=[pltpu.VMEM((flat, nz), jnp.float32)],
    )
    fx_b, div = lax.optimization_barrier((fx_b, div))
    gx_b, total = second(fx_b, total, "gx")

    args = [forcing, target_flux, vel_xy, uz, div, slope, total, gx_a, gx_b]
    vel_new, source, forcing_new = call(
        functools.partial(finish_kernel, cells),
        args, [smem, smem, any_space] + [None] * (len(args) - 3),
        [f32(3, nx, ny, nz), cube, f32(1)], [one(2), None, smem], "finish",
        input_output_aliases={2: 0},
    )
    return vel_new, source, forcing_new


def solution(mesh):
    return jax.shard_map(
        local,
        mesh=mesh,
        in_specs=(
            P(None, "gx", "gy", "gz"),
            P("gx", "gy", "gz"),
            P("gx", "gy", "gz"),
            P(None, "gx", "gy", "gz"),
            P(),
            P(),
        ),
        out_specs=(P(None, "gx", "gy", "gz"), P("gx", "gy", "gz"), P()),
        check_vma=False,
    )
```

```python
import functools
import math

import jax
import jax.numpy as jnp
from jax import lax
from jax.experimental import pallas as pl
from jax.experimental.pallas import tpu as pltpu
from jax.sharding import PartitionSpec as P

time_step = 0.2
viscosity = 0.1
drag_scale = 1.0

PARAMS = pltpu.CompilerParams(vmem_limit_bytes=16 * 2**20)


def pairs_a(count):
    return [(i, i ^ 1) for i in range(count)]


def pairs_b(count):
    swaps = []
    for i in range(1, count, 2):
        swaps += [(i, (i + 1) % count), ((i + 1) % count, i)]
    return swaps


def even(axis):
    return lax.axis_index(axis) % 2 == 0


def z_rows(field):
    return field.T


def pack_kernel(
    vel_hbm, pres_hbm, void_hbm, x_a, x_b, y_a, y_b, z_a, z_b, columns, vel, pres, void, sems
):
    copies = [
        pltpu.make_async_copy(src, dst, sems.at[k])
        for k, (src, dst) in enumerate(((vel_hbm, vel), (pres_hbm, pres), (void_hbm, void)))
    ]
    for copy in copies:
        copy.start()
    for copy in copies:
        copy.wait()
    _, nx, ny, nz = vel.shape
    x_even, y_even, z_even = even("gx"), even("gy"), even("gz")
    for out, at in ((x_a, jnp.where(x_even, nx - 1, 0)), (x_b, jnp.where(x_even, 0, nx - 1))):
        for c in range(3):
            out[c] = vel[c, at]
        out[3] = pres[at]
    at_a, at_b = jnp.where(y_even, ny - 1, 0), jnp.where(y_even, 0, ny - 1)
    lane = lax.broadcasted_iota(jnp.int32, (ny, nz), 1)

    def slab(i, carry):
        for out, at in ((y_a, at_a), (y_b, at_b)):
            if out is not None:
                for c in range(3):
                    out[c, pl.ds(i, 1), :] = vel[c, i, pl.ds(at, 1), :]
                out[3, pl.ds(i, 1), :] = pres[i, pl.ds(at, 1), :]
        fields = [vel[0, i], vel[1, i], vel[2, i], pres[i], void[i]]
        joined = pltpu.roll(fields[0], 1, 1)
        for f in range(1, 5):
            joined = jnp.where(lane >= 2 * f, pltpu.roll(fields[f], 2 * f + 1, 1), joined)
        columns[pl.ds(pl.multiple_of(i * ny, ny), ny), :] = joined
        return carry

    lax.fori_loop(0, nx, slab, 0, unroll=4)
    rows = z_rows(columns[...])
    for f in range(5):
        high, low = rows[2 * f : 2 * f + 1], rows[2 * f + 1 : 2 * f + 2]
        z_a[f : f + 1, :] = jnp.where(z_even, high, low)
        z_b[f : f + 1, :] = jnp.where(z_even, low, high)
    for out in (z_a, z_b):
        out[5:8, :] = jnp.zeros((3, out.shape[1]), jnp.float32)


def drag_kernel(vel, void, part, rate, scale, void_part):
    _, nx, ny, nz = vel.shape

    def slab(i, acc):
        eps = void[i]
        slip2 = sum((vel[c, i] - part[c, i]) ** 2 for c in range(3))
        here = drag_scale * (1.0 - eps) * jnp.exp(-2.65 * jnp.log(eps)) * (1.0 + jnp.sqrt(slip2))
        rate[i] = time_step * here
        scale[i] = 1.0 / (1.0 + time_step * here)
        return acc + eps

    acc = lax.fori_loop(0, nx, slab, jnp.zeros((ny, nz), jnp.float32), unroll=4)
    void_part[...] = column_sum(acc)


def column_sum(value):
    return jnp.sum(value, axis=0, keepdims=True)


class Stencil:
    def __init__(self, vel, pres, halo, x_a, x_b, y_a, y_b):
        _, self.nx, self.ny, self.nz = vel.shape
        self.vel, self.pres, self.halo = vel, pres, halo
        self.x, self.y = (x_a, x_b), (y_a, y_b)
        self.x_even, self.y_even = even("gx"), even("gy")
        xi, yi = lax.axis_index("gx"), lax.axis_index("gy")
        self.x_low, self.x_high = xi == 0, xi == lax.axis_size("gx") - 1
        self.y_low, self.y_high = yi == 0, yi == lax.axis_size("gy") - 1
        self.lane = lax.broadcasted_iota(jnp.int32, (self.ny, self.nz), 1)
        self.row = lax.broadcasted_iota(jnp.int32, (self.ny, self.nz), 0)

    def load(self, f, i):
        return self.vel[f, i] if f < 3 else self.pres[i]

    def along_x(self, f, i, first, last):
        a, b = self.x
        if first:
            wall = 0.0 if f < 3 else self.pres[0]
            low = jnp.where(self.x_low, wall, jnp.where(self.x_even, b[f], a[f]))
        else:
            low = self.load(f, i - 1)
        if last:
            wall = 0.0 if f < 3 else self.pres[self.nx - 1]
            high = jnp.where(self.x_high, wall, jnp.where(self.x_even, a[f], b[f]))
        else:
            high = self.load(f, i + 1)
        return low, high

    def along_y(self, f, i):
        here = self.load(f, i)
        row_a = self.y[0][f, pl.ds(i, 1), :]
        row_b = self.y[1][f, pl.ds(i, 1), :] if self.y[1] is not None else row_a
        wall_low = 0.0 if f < 3 else here[0:1]
        wall_high = 0.0 if f < 3 else here[self.ny - 1 : self.ny]
        low = jnp.where(self.y_low, wall_low, jnp.where(self.y_even, row_b, row_a))
        high = jnp.where(self.y_high, wall_high, jnp.where(self.y_even, row_a, row_b))
        return (
            jnp.where(self.row == 0, low, pltpu.roll(here, 1, 0)),
            jnp.where(self.row == self.ny - 1, high, pltpu.roll(here, self.ny - 1, 0)),
        )

    def rows_at(self, i):
        return pl.ds(i * self.ny if isinstance(i, int) else pl.multiple_of(i * self.ny, self.ny), self.ny)

    def along_z(self, here, f, i):
        edge = self.halo[self.rows_at(i), :]
        low = jnp.where(self.lane == 0, edge[:, f : f + 1], pltpu.roll(here, 1, 1))
        high = jnp.where(
            self.lane == self.nz - 1, edge[:, 8 + f : 9 + f], pltpu.roll(here, self.nz - 1, 1)
        )
        return low, high

    def ustar(self, c, i, first, last, part, rate, scale, push):
        here = self.load(c, i)
        xm, xp = self.along_x(c, i, first, last)
        ym, yp = self.along_y(c, i)
        zm, zp = self.along_z(here, c, i)
        u = [self.load(d, i) for d in range(3)]
        advection = (u[0] * (xp - xm) + u[1] * (yp - ym) + u[2] * (zp - zm)) * 0.5
        laplace = (xm + xp) + (ym + yp) + (zm + zp) - 6.0 * here
        if c == 0:
            pm, pp = self.along_x(3, i, first, last)
        elif c == 1:
            pm, pp = self.along_y(3, i)
        else:
            pm, pp = self.along_z(self.load(3, i), 3, i)
        force = viscosity * laplace - advection - (pp - pm) * 0.5
        if push is not None:
            force = force + push
        return (here + time_step * force + rate[i] * part[i]) * scale[i]


def sweep(nx, slab, acc, unroll=4):
    acc = slab(0, True, False, acc)
    inner = (nx - 2) // unroll * unroll
    acc = lax.fori_loop(1, 1 + inner, lambda i, a: slab(i, False, False, a), acc, unroll=unroll)
    for i in range(1 + inner, nx - 1):
        acc = slab(i, False, False, acc)
    return slab(nx - 1, False, True, acc)


def z_kernel(
    forcing, vel, pres, void, part, rate, scale, void_part, x_a, x_b, y_a, y_b, z_a, z_b,
    uz, flux, slope, fz_a, fz_b, sums, halo,
):
    _, nx, ny, nz = vel.shape
    z_even = even("gz")
    low_rows = jnp.where(z_even, z_b[...], z_a[...])
    high_rows = jnp.where(z_even, z_a[...], z_b[...])
    halo[...] = jnp.concatenate(
        [low_rows, high_rows, jnp.zeros((nz - 16, low_rows.shape[1]), jnp.float32)], axis=0
    ).T
    near = Stencil(vel, pres, halo, x_a, x_b, y_a, y_b)
    push = forcing[0]

    def slab(i, first, last, acc):
        value = near.ustar(2, i, first, last, part.at[0], rate, scale, push)
        uz[i] = value
        eps = void[i]
        em, ep = near.along_z(eps, 4, i)
        slope[i] = (ep - em) * 0.5
        flow = eps * value
        flux[near.rows_at(i), :] = flow
        return acc + flow

    acc = sweep(nx, slab, jnp.zeros((ny, nz), jnp.float32))
    face_rows = nx * ny // nz
    sums[...] = jnp.zeros(sums.shape, jnp.float32)
    sums[face_rows : face_rows + 1] = column_sum(acc)
    sums[face_rows + 1 : face_rows + 2] = void_part[...]
    turned = z_rows(flux[...])
    z_low, z_high = turned[0:1], turned[nz - 1 : nz]
    send_a, send_b = jnp.where(z_even, z_high, z_low), jnp.where(z_even, z_low, z_high)
    fz_a[...] = sums[...]
    fz_b[...] = jnp.zeros(fz_b.shape, jnp.float32)
    for out, send in ((fz_a, send_a), (fz_b, send_b)):
        for k in range(face_rows):
            out[k : k + 1, :] = send[:, k * nz : (k + 1) * nz]


def y_kernel(
    vel, pres, void, part, rate, scale, flux_z, halo, x_a, x_b, y_a, y_b,
    out, div, fy_a, fy_b,
):
    _, nx, ny, nz = vel.shape
    near = Stencil(vel, pres, halo, x_a, x_b, y_a, y_b)

    def slab(i, first, last, acc):
        value = near.ustar(1, i, first, last, part.at[0], rate, scale, None)
        out[i] = value
        flow = void[i] * value
        ym = jnp.where(near.row == 0, 0.0, pltpu.roll(flow, 1, 0))
        yp = jnp.where(near.row == ny - 1, 0.0, pltpu.roll(flow, ny - 1, 0))
        up = flux_z[near.rows_at(i), :]
        zm = jnp.where(near.lane == 0, 0.0, pltpu.roll(up, 1, 1))
        zp = jnp.where(near.lane == nz - 1, 0.0, pltpu.roll(up, nz - 1, 1))
        div[i] = ((yp - ym) + (zp - zm)) * 0.5
        first_row, last_row = flow[0:1], flow[ny - 1 : ny]
        fy_a[pl.ds(i, 1), :] = jnp.where(near.y_even, last_row, first_row)
        if fy_b is not None:
            fy_b[pl.ds(i, 1), :] = jnp.where(near.y_even, first_row, last_row)
        return acc

    sweep(nx, slab, 0)


def x_kernel(
    vel, pres, void, part, rate, scale, halo, div_yz, x_a, x_b, y_a, y_b,
    out, div, fx_a, fx_b, flux,
):
    _, nx, ny, nz = vel.shape
    near = Stencil(vel, pres, halo, x_a, x_b, y_a, y_b)

    def slab(i, first, last, acc):
        value = near.ustar(0, i, first, last, part.at[0], rate, scale, None)
        out[i] = value
        flux[i] = void[i] * value
        return acc

    sweep(nx, slab, 0)

    def join(i, first, last, acc):
        low = 0.0 if first else flux[i - 1]
        high = 0.0 if last else flux[i + 1]
        div[i] = div_yz[i] + (high - low) * 0.5
        return acc

    sweep(nx, join, 0)
    low, high = flux[0], flux[nx - 1]
    fx_a[...] = jnp.where(near.x_even, high, low)
    fx_b[...] = jnp.where(near.x_even, low, high)


def edge_kernel(div, fy_a, fy_b, fz_a, fz_b, out, halo):
    nx, ny, nz = div.shape
    y_even, z_even = even("gy"), even("gz")
    yi = lax.axis_index("gy")
    y_low, y_high = yi == 0, yi == lax.axis_size("gy") - 1
    a, b = (
        jnp.concatenate([face[k : k + 1] for k in range(nx * ny // nz)], axis=1)
        for face in (fz_a, fz_b)
    )
    low_row, high_row = jnp.where(z_even, b, a), jnp.where(z_even, a, b)
    pick = lax.broadcasted_iota(jnp.int32, (nz, halo.shape[0]), 0)
    halo[...] = jnp.where(pick == 0, -low_row, jnp.where(pick == nz - 1, high_row, 0.0)).T
    row = lax.broadcasted_iota(jnp.int32, (ny, nz), 0)

    def slab(i, carry):
        rows_at = pl.ds(pl.multiple_of(i * ny, ny), ny)
        row_a = fy_a[pl.ds(i, 1), :]
        row_b = fy_b[pl.ds(i, 1), :] if fy_b is not None else row_a
        ym = jnp.where(y_low, 0.0, jnp.where(y_even, row_b, row_a))
        yp = jnp.where(y_high, 0.0, jnp.where(y_even, row_a, row_b))
        ends = jnp.where(row == 0, -ym, jnp.where(row == ny - 1, yp, 0.0)) + halo[rows_at, :]
        out[i] = div[i] + 0.5 * ends
        return carry

    lax.fori_loop(0, nx, slab, 0, unroll=4)


def copy_kernel(ux, uy, out, sems):
    copies = [
        pltpu.make_async_copy(value, out.at[c], sems.at[c]) for c, value in enumerate((ux, uy))
    ]
    for copy in copies:
        copy.start()
    for copy in copies:
        copy.wait()


def finish_kernel(
    cells, forcing, target, kept, uz, div, slope, sums, fx_a, fx_b, vel_new, source, forcing_new
):
    nx, ny, nz = div.shape
    x_even = even("gx")
    xi = lax.axis_index("gx")
    x_low, x_high = xi == 0, xi == lax.axis_size("gx") - 1
    row = nx * ny // nz
    flow, total = jnp.sum(sums[row : row + 1]), jnp.sum(sums[row + 1 : row + 2])
    step = (target[0] * cells - flow) / (time_step * total)
    forcing_new[0] = forcing[0] + step
    rise = time_step * step
    xl = jnp.where(x_low, 0.0, jnp.where(x_even, fx_b[0:ny], fx_a[0:ny]))
    xh = jnp.where(x_high, 0.0, jnp.where(x_even, fx_a[0:ny], fx_b[0:ny]))

    def slab(i, first, last, acc):
        value = div[i] + rise * slope[i]
        if first:
            value = value - 0.5 * xl
        if last:
            value = value + 0.5 * xh
        source[i] = value
        vel_new[0, i] = uz[i] + rise
        return acc

    sweep(nx, slab, 0)


def swap(value, axis, second=False):
    count = lax.axis_size(axis)
    return lax.ppermute(value, axis, pairs_b(count) if second else pairs_a(count))


def optional(kernel, slots):
    def run(*refs):
        refs = list(refs)
        for slot in slots:
            refs.insert(slot, None)
        return kernel(*refs)

    return run


def f32(*shape):
    return jax.ShapeDtypeStruct(shape, jnp.float32)


def local(velocity, pressure, voidage, particle_vel, forcing, target_flux):
    _, nx, ny, nz = velocity.shape
    counts = {axis: lax.axis_size(axis) for axis in ("gx", "gy", "gz")}
    cells = float(voidage.size * math.prod(counts.values()))
    two_y = counts["gy"] > 2
    flat = nx * ny
    smem = pl.BlockSpec(memory_space=pltpu.SMEM)
    vmem = pl.BlockSpec(memory_space=pltpu.VMEM)

    any_space = pl.BlockSpec(memory_space=pl.ANY)
    y_out = [f32(4, nx, nz)] * (2 if two_y else 1)
    faces = pl.pallas_call(
        optional(pack_kernel, () if two_y else (6,)),
        out_shape=[f32(4, ny, nz), f32(4, ny, nz)] + y_out + [f32(8, flat)] * 2,
        in_specs=[pl.BlockSpec(memory_space=pltpu.HBM)] * 3,
        scratch_shapes=[pltpu.VMEM((flat, nz), jnp.float32)]
        + [pltpu.VMEM(v.shape, jnp.float32) for v in (velocity, pressure, voidage)]
        + [pltpu.SemaphoreType.DMA((3,))],
        compiler_params=pltpu.CompilerParams(vmem_limit_bytes=61000 * 2**10),
        name="pack",
    )(velocity, pressure, voidage)
    x_a, x_b, *y_faces, z_a, z_b = faces
    near = [swap(x_a, "gx"), swap(x_b, "gx", True)]
    near += [swap(y, "gy", k == 1) for k, y in enumerate(y_faces)]
    z_near = [swap(z_a, "gz"), swap(z_b, "gz", True)]

    cube = f32(nx, ny, nz)
    rate, scale, void_part = pl.pallas_call(
        drag_kernel,
        out_shape=[cube, cube, f32(1, nz)],
        in_specs=[vmem] * 3,
        compiler_params=PARAMS,
        name="drag",
    )(velocity, voidage, particle_vel)

    def whole(value):
        return pl.BlockSpec(value.shape, lambda i: (0,) * len(value.shape))

    def one(c):
        return pl.BlockSpec((1, nx, ny, nz), lambda i: (c, 0, 0, 0))

    def call(kernel, args, specs, outs, out_specs, name, **more):
        return pl.pallas_call(
            kernel,
            grid=(1,),
            in_specs=[whole(v) if spec is None else spec for v, spec in zip(args, specs)],
            out_shape=outs,
            out_specs=[whole(v) if spec is None else spec for v, spec in zip(outs, out_specs)],
            compiler_params=PARAMS,
            name=name,
            **more,
        )(*args)

    args = [forcing, velocity, pressure, voidage, particle_vel, rate, scale, void_part, *near, *z_near]
    face_rows = flat // nz
    tile = f32(-(-(face_rows + 2) // 8) * 8, nz)
    outs = [cube, f32(flat, nz), cube, tile, tile, tile, f32(flat, nz)]
    uz, flux_z, slope, fz_a, fz_b, sums, halo = call(
        optional(z_kernel, () if two_y else (11,)),
        args, [smem, None, None, None, one(2)] + [None] * (len(args) - 5), outs, [None] * len(outs), "z",
    )
    gz_a = swap(fz_a, "gz")

    args = [velocity, pressure, voidage, particle_vel, rate, scale, flux_z, halo, *near]
    outs = [cube, cube] + [f32(nx, nz)] * len(y_faces)
    uy, div_yz, *fy = call(
        optional(y_kernel, () if two_y else (11, 15)),
        args, [None, None, None, one(1)] + [None] * (len(args) - 4),
        outs, [None] * len(outs), "y",
    )
    fz_b, fy[0] = lax.optimization_barrier((fz_b, fy[0]))

    in_sums = lax.broadcasted_iota(jnp.int32, tile.shape, 0) >= face_rows

    def z_total(value):
        return jnp.where(in_sums, value, 0.0)

    def reduce_rest(total, axis):
        step = 2
        while counts[axis] > 4 and step < counts[axis]:
            swaps = [(i, i ^ step) for i in range(counts[axis])]
            total = total + lax.ppermute(total, axis, swaps)
            step *= 2
        return total

    def second(face, total, axis):
        got = swap(jnp.concatenate([face, total]), axis, True)
        if counts[axis] == 4:
            total = total + got[-tile.shape[0] :]
        return got, reduce_rest(total, axis)

    total = sums + z_total(gz_a)
    gz_b = swap(fz_b + total, "gz", True)

    args = [velocity, pressure, voidage, particle_vel, rate, scale, halo, div_yz, *near]
    outs = [cube, cube, f32(ny, nz), f32(ny, nz)]
    ux, div, fx_a, fx_b = call(
        optional(x_kernel, () if two_y else (11,)),
        args, [None, None, None, one(0)] + [None] * (len(args) - 4),
        outs, [None] * 4, "x",
        scratch_shapes=[pltpu.VMEM((nx, ny, nz), jnp.float32)],
    )
    if counts["gz"] == 4:
        total = total + z_total(gz_b)
    total = reduce_rest(total, "gz")

    face, fx_a, fx_b = lax.optimization_barrier((fy[0], fx_a, fx_b))
    gy = [swap(jnp.concatenate([face, total]), "gy")]
    total = total + gy[0][-tile.shape[0] :]
    if two_y:
        got, total = second(fy[1], total, "gy")
        gy.append(got)

    vel_xy = pl.pallas_call(
        copy_kernel,
        out_shape=f32(3, nx, ny, nz),
        in_specs=[vmem] * 2,
        out_specs=any_space,
        scratch_shapes=[pltpu.SemaphoreType.DMA((2,))],
        compiler_params=PARAMS,
        name="copy_xy",
    )(ux, uy)
    fx_a, vel_xy = lax.optimization_barrier((fx_a, vel_xy))
    gx_a = swap(jnp.concatenate([fx_a, total]), "gx")
    total = total + gx_a[-tile.shape[0] :]
    args = [div, *gy, gz_a, gz_b]
    (div,) = call(
        optional(edge_kernel, () if two_y else (2,)),
        args, [None] * len(args), [cube], [None], "edge",
        scratch_shapes=[pltpu.VMEM((flat, nz), jnp.float32)],
    )
    fx_b, div = lax.optimization_barrier((fx_b, div))
    gx_b, total = second(fx_b, total, "gx")

    args = [forcing, target_flux, vel_xy, uz, div, slope, total, gx_a, gx_b]
    vel_new, source, forcing_new = call(
        functools.partial(finish_kernel, cells),
        args, [smem, smem, any_space] + [None] * (len(args) - 3),
        [f32(3, nx, ny, nz), cube, f32(1)], [one(2), None, smem], "finish",
        input_output_aliases={2: 0},
    )
    return vel_new, source, forcing_new


def solution(mesh):
    return jax.shard_map(
        local,
        mesh=mesh,
        in_specs=(
            P(None, "gx", "gy", "gz"),
            P("gx", "gy", "gz"),
            P("gx", "gy", "gz"),
            P(None, "gx", "gy", "gz"),
            P(),
            P(),
        ),
        out_specs=(P(None, "gx", "gy", "gz"), P("gx", "gy", "gz"), P()),
        check_vma=False,
    )
```

```python
import functools
import math

import jax
import jax.numpy as jnp
from jax import lax
from jax.experimental import pallas as pl
from jax.experimental.pallas import tpu as pltpu
from jax.sharding import PartitionSpec as P


time_step = 0.2
viscosity = 0.1
drag_scale = 1.0

PARAMS = pltpu.CompilerParams(vmem_limit_bytes=16 * 2**20)


def pairs_a(count):
    return [(i, i ^ 1) for i in range(count)]


def pairs_b(count):
    swaps = []
    for i in range(1, count, 2):
        swaps += [(i, (i + 1) % count), ((i + 1) % count, i)]
    return swaps


def even(axis):
    return lax.axis_index(axis) % 2 == 0


def z_rows(field):
    return field.T


def pack_x_kernel(vel, pres, x_a, x_b, sems):
    nx = vel.shape[1]
    x_even = even("gx")
    copies = []
    for k, (out, at) in enumerate(
        ((x_a, jnp.where(x_even, nx - 1, 0)), (x_b, jnp.where(x_even, 0, nx - 1)))
    ):
        for c in range(3):
            copies.append(pltpu.make_async_copy(vel.at[c, at], out.at[c], sems.at[k, c]))
        copies.append(pltpu.make_async_copy(pres.at[at], out.at[3], sems.at[k, 3]))
    for copy in copies:
        copy.start()
    for copy in copies:
        copy.wait()


def pack_kernel(vel, pres, void, y_a, y_b, z_a, z_b, columns):
    _, nx, ny, nz = vel.shape
    y_even, z_even = even("gy"), even("gz")
    at_a, at_b = jnp.where(y_even, ny - 1, 0), jnp.where(y_even, 0, ny - 1)
    lane = lax.broadcasted_iota(jnp.int32, (ny, nz), 1)

    def slab(i, carry):
        for out, at in ((y_a, at_a), (y_b, at_b)):
            if out is not None:
                for c in range(3):
                    out[c, pl.ds(i, 1), :] = vel[c, i, pl.ds(at, 1), :]
                out[3, pl.ds(i, 1), :] = pres[i, pl.ds(at, 1), :]
        fields = [vel[0, i], vel[1, i], vel[2, i], pres[i], void[i]]
        joined = pltpu.roll(fields[0], 1, 1)
        for f in range(1, 5):
            joined = jnp.where(lane >= 2 * f, pltpu.roll(fields[f], 2 * f + 1, 1), joined)
        columns[pl.ds(pl.multiple_of(i * ny, ny), ny), :] = joined
        return carry

    lax.fori_loop(0, nx, slab, 0, unroll=4)
    rows = z_rows(columns[...])
    for f in range(5):
        high, low = rows[2 * f : 2 * f + 1], rows[2 * f + 1 : 2 * f + 2]
        z_a[f : f + 1, :] = jnp.where(z_even, high, low)
        z_b[f : f + 1, :] = jnp.where(z_even, low, high)
    for out in (z_a, z_b):
        out[5:8, :] = jnp.zeros((3, out.shape[1]), jnp.float32)


def drag_kernel(vel, void, part, rate, scale, void_part):
    _, nx, ny, nz = vel.shape

    def slab(i, acc):
        eps = void[i]
        slip2 = sum((vel[c, i] - part[c, i]) ** 2 for c in range(3))
        here = drag_scale * (1.0 - eps) * jnp.exp(-2.65 * jnp.log(eps)) * (1.0 + jnp.sqrt(slip2))
        rate[i] = time_step * here
        scale[i] = 1.0 / (1.0 + time_step * here)
        return acc + eps

    acc = lax.fori_loop(0, nx, slab, jnp.zeros((ny, nz), jnp.float32), unroll=4)
    void_part[...] = column_sum(acc)


def column_sum(value):
    return jnp.sum(value, axis=0, keepdims=True)


class Stencil:
    def __init__(self, vel, pres, halo, x_a, x_b, y_a, y_b):
        _, self.nx, self.ny, self.nz = vel.shape
        self.vel, self.pres, self.halo = vel, pres, halo
        self.x, self.y = (x_a, x_b), (y_a, y_b)
        self.x_even, self.y_even = even("gx"), even("gy")
        xi, yi = lax.axis_index("gx"), lax.axis_index("gy")
        self.x_low, self.x_high = xi == 0, xi == lax.axis_size("gx") - 1
        self.y_low, self.y_high = yi == 0, yi == lax.axis_size("gy") - 1
        self.lane = lax.broadcasted_iota(jnp.int32, (self.ny, self.nz), 1)
        self.row = lax.broadcasted_iota(jnp.int32, (self.ny, self.nz), 0)

    def load(self, f, i):
        return self.vel[f, i] if f < 3 else self.pres[i]

    def along_x(self, f, i, first, last):
        a, b = self.x
        if first:
            wall = 0.0 if f < 3 else self.pres[0]
            low = jnp.where(self.x_low, wall, jnp.where(self.x_even, b[f], a[f]))
        else:
            low = self.load(f, i - 1)
        if last:
            wall = 0.0 if f < 3 else self.pres[self.nx - 1]
            high = jnp.where(self.x_high, wall, jnp.where(self.x_even, a[f], b[f]))
        else:
            high = self.load(f, i + 1)
        return low, high

    def along_y(self, f, i):
        here = self.load(f, i)
        row_a = self.y[0][f, pl.ds(i, 1), :]
        row_b = self.y[1][f, pl.ds(i, 1), :] if self.y[1] is not None else row_a
        wall_low = 0.0 if f < 3 else here[0:1]
        wall_high = 0.0 if f < 3 else here[self.ny - 1 : self.ny]
        low = jnp.where(self.y_low, wall_low, jnp.where(self.y_even, row_b, row_a))
        high = jnp.where(self.y_high, wall_high, jnp.where(self.y_even, row_a, row_b))
        return (
            jnp.where(self.row == 0, low, pltpu.roll(here, 1, 0)),
            jnp.where(self.row == self.ny - 1, high, pltpu.roll(here, self.ny - 1, 0)),
        )

    def rows_at(self, i):
        return pl.ds(i * self.ny if isinstance(i, int) else pl.multiple_of(i * self.ny, self.ny), self.ny)

    def along_z(self, here, f, i):
        edge = self.halo[self.rows_at(i), :]
        low = jnp.where(self.lane == 0, edge[:, f : f + 1], pltpu.roll(here, 1, 1))
        high = jnp.where(
            self.lane == self.nz - 1, edge[:, 8 + f : 9 + f], pltpu.roll(here, self.nz - 1, 1)
        )
        return low, high

    def ustar(self, c, i, first, last, part, rate, scale, push):
        here = self.load(c, i)
        xm, xp = self.along_x(c, i, first, last)
        ym, yp = self.along_y(c, i)
        zm, zp = self.along_z(here, c, i)
        u = [self.load(d, i) for d in range(3)]
        advection = (u[0] * (xp - xm) + u[1] * (yp - ym) + u[2] * (zp - zm)) * 0.5
        laplace = (xm + xp) + (ym + yp) + (zm + zp) - 6.0 * here
        if c == 0:
            pm, pp = self.along_x(3, i, first, last)
        elif c == 1:
            pm, pp = self.along_y(3, i)
        else:
            pm, pp = self.along_z(self.load(3, i), 3, i)
        force = viscosity * laplace - advection - (pp - pm) * 0.5
        if push is not None:
            force = force + push
        return (here + time_step * force + rate[i] * part[i]) * scale[i]


def sweep(nx, slab, acc, unroll=4):
    acc = slab(0, True, False, acc)
    inner = (nx - 2) // unroll * unroll
    acc = lax.fori_loop(1, 1 + inner, lambda i, a: slab(i, False, False, a), acc, unroll=unroll)
    for i in range(1 + inner, nx - 1):
        acc = slab(i, False, False, acc)
    return slab(nx - 1, False, True, acc)


def z_kernel(
    forcing, vel, pres, void, part, rate, scale, void_part, x_a, x_b, y_a, y_b, z_a, z_b,
    uz, flux, slope, fz_a, fz_b, sums, halo,
):
    _, nx, ny, nz = vel.shape
    z_even = even("gz")
    low_rows = jnp.where(z_even, z_b[...], z_a[...])
    high_rows = jnp.where(z_even, z_a[...], z_b[...])
    halo[...] = jnp.concatenate(
        [low_rows, high_rows, jnp.zeros((nz - 16, low_rows.shape[1]), jnp.float32)], axis=0
    ).T
    near = Stencil(vel, pres, halo, x_a, x_b, y_a, y_b)
    push = forcing[0]

    def slab(i, first, last, acc):
        value = near.ustar(2, i, first, last, part.at[0], rate, scale, push)
        uz[i] = value
        eps = void[i]
        em, ep = near.along_z(eps, 4, i)
        slope[i] = (ep - em) * 0.5
        flow = eps * value
        flux[near.rows_at(i), :] = flow
        return acc + flow

    acc = sweep(nx, slab, jnp.zeros((ny, nz), jnp.float32))
    face_rows = nx * ny // nz
    sums[...] = jnp.zeros(sums.shape, jnp.float32)
    sums[face_rows : face_rows + 1] = column_sum(acc)
    sums[face_rows + 1 : face_rows + 2] = void_part[...]
    turned = z_rows(flux[...])
    z_low, z_high = turned[0:1], turned[nz - 1 : nz]
    send_a, send_b = jnp.where(z_even, z_high, z_low), jnp.where(z_even, z_low, z_high)
    fz_a[...] = sums[...]
    fz_b[...] = jnp.zeros(fz_b.shape, jnp.float32)
    for out, send in ((fz_a, send_a), (fz_b, send_b)):
        for k in range(face_rows):
            out[k : k + 1, :] = send[:, k * nz : (k + 1) * nz]


def y_kernel(
    vel, pres, void, part, rate, scale, flux_z, halo, x_a, x_b, y_a, y_b,
    out, div, fy_a, fy_b,
):
    _, nx, ny, nz = vel.shape
    near = Stencil(vel, pres, halo, x_a, x_b, y_a, y_b)

    def slab(i, first, last, acc):
        value = near.ustar(1, i, first, last, part.at[0], rate, scale, None)
        out[i] = value
        flow = void[i] * value
        ym = jnp.where(near.row == 0, 0.0, pltpu.roll(flow, 1, 0))
        yp = jnp.where(near.row == ny - 1, 0.0, pltpu.roll(flow, ny - 1, 0))
        up = flux_z[near.rows_at(i), :]
        zm = jnp.where(near.lane == 0, 0.0, pltpu.roll(up, 1, 1))
        zp = jnp.where(near.lane == nz - 1, 0.0, pltpu.roll(up, nz - 1, 1))
        div[i] = ((yp - ym) + (zp - zm)) * 0.5
        first_row, last_row = flow[0:1], flow[ny - 1 : ny]
        fy_a[pl.ds(i, 1), :] = jnp.where(near.y_even, last_row, first_row)
        if fy_b is not None:
            fy_b[pl.ds(i, 1), :] = jnp.where(near.y_even, first_row, last_row)
        return acc

    sweep(nx, slab, 0)


def x_kernel(
    vel, pres, void, part, rate, scale, halo, div_yz, x_a, x_b, y_a, y_b,
    out, div, fx_a, fx_b, flux,
):
    _, nx, _, _ = vel.shape
    near = Stencil(vel, pres, halo, x_a, x_b, y_a, y_b)

    def slab(i, first, last, acc):
        value = near.ustar(0, i, first, last, part.at[0], rate, scale, None)
        out[i] = value
        flux[i] = void[i] * value
        return acc

    sweep(nx, slab, 0)

    def join(i, first, last, acc):
        low = 0.0 if first else flux[i - 1]
        high = 0.0 if last else flux[i + 1]
        div[i] = div_yz[i] + (high - low) * 0.5
        return acc

    sweep(nx, join, 0)
    low, high = flux[0], flux[nx - 1]
    fx_a[...] = jnp.where(near.x_even, high, low)
    fx_b[...] = jnp.where(near.x_even, low, high)


def edge_kernel(div, fy_a, fy_b, fz_a, fz_b, out, halo):
    nx, ny, nz = div.shape
    y_even, z_even = even("gy"), even("gz")
    yi = lax.axis_index("gy")
    y_low, y_high = yi == 0, yi == lax.axis_size("gy") - 1
    a, b = (
        jnp.concatenate([face[k : k + 1] for k in range(nx * ny // nz)], axis=1)
        for face in (fz_a, fz_b)
    )
    low_row, high_row = jnp.where(z_even, b, a), jnp.where(z_even, a, b)
    pick = lax.broadcasted_iota(jnp.int32, (nz, halo.shape[0]), 0)
    halo[...] = jnp.where(pick == 0, -low_row, jnp.where(pick == nz - 1, high_row, 0.0)).T
    row = lax.broadcasted_iota(jnp.int32, (ny, nz), 0)

    def slab(i, carry):
        rows_at = pl.ds(pl.multiple_of(i * ny, ny), ny)
        row_a = fy_a[pl.ds(i, 1), :]
        row_b = fy_b[pl.ds(i, 1), :] if fy_b is not None else row_a
        ym = jnp.where(y_low, 0.0, jnp.where(y_even, row_b, row_a))
        yp = jnp.where(y_high, 0.0, jnp.where(y_even, row_a, row_b))
        ends = jnp.where(row == 0, -ym, jnp.where(row == ny - 1, yp, 0.0)) + halo[rows_at, :]
        out[i] = div[i] + 0.5 * ends
        return carry

    lax.fori_loop(0, nx, slab, 0, unroll=4)


def copy_kernel(ux, uy, out, sems):
    copies = [
        pltpu.make_async_copy(value, out.at[c], sems.at[c]) for c, value in enumerate((ux, uy))
    ]
    for copy in copies:
        copy.start()
    for copy in copies:
        copy.wait()


def finish_kernel(
    cells, forcing, target, kept, uz, div, slope, sums, fx_a, fx_b, vel_new, source, forcing_new
):
    nx, ny, nz = div.shape
    x_even = even("gx")
    xi = lax.axis_index("gx")
    x_low, x_high = xi == 0, xi == lax.axis_size("gx") - 1
    row = nx * ny // nz
    flow, total = jnp.sum(sums[row : row + 1]), jnp.sum(sums[row + 1 : row + 2])
    step = (target[0] * cells - flow) / (time_step * total)
    forcing_new[0] = forcing[0] + step
    rise = time_step * step
    xl = jnp.where(x_low, 0.0, jnp.where(x_even, fx_b[0:ny], fx_a[0:ny]))
    xh = jnp.where(x_high, 0.0, jnp.where(x_even, fx_a[0:ny], fx_b[0:ny]))

    def slab(i, first, last, acc):
        value = div[i] + rise * slope[i]
        if first:
            value = value - 0.5 * xl
        if last:
            value = value + 0.5 * xh
        source[i] = value
        vel_new[0, i] = uz[i] + rise
        return acc

    sweep(nx, slab, 0)


def swap(value, axis, second=False):
    count = lax.axis_size(axis)
    return lax.ppermute(value, axis, pairs_b(count) if second else pairs_a(count))


def optional(kernel, slots):
    def run(*refs):
        refs = list(refs)
        for slot in slots:
            refs.insert(slot, None)
        return kernel(*refs)

    return run


def f32(*shape):
    return jax.ShapeDtypeStruct(shape, jnp.float32)


def local(velocity, pressure, voidage, particle_vel, forcing, target_flux):
    _, nx, ny, nz = velocity.shape
    counts = {axis: lax.axis_size(axis) for axis in ("gx", "gy", "gz")}
    cells = float(voidage.size * math.prod(counts.values()))
    two_y = counts["gy"] > 2
    flat = nx * ny
    smem = pl.BlockSpec(memory_space=pltpu.SMEM)
    vmem = pl.BlockSpec(memory_space=pltpu.VMEM)

    any_space = pl.BlockSpec(memory_space=pl.ANY)
    y_out = [f32(4, nx, nz)] * (2 if two_y else 1)
    x_a, x_b = pl.pallas_call(
        pack_x_kernel,
        out_shape=[f32(4, ny, nz)] * 2,
        in_specs=[pl.BlockSpec(memory_space=pltpu.HBM)] * 2,
        scratch_shapes=[pltpu.SemaphoreType.DMA((2, 4))],
        compiler_params=pltpu.CompilerParams(vmem_limit_bytes=61000 * 2**10),
        name="pack_x",
    )(velocity, pressure)
    near = [swap(x_a, "gx")]
    near.append(swap(x_b, "gx", True))
    x_a, x_b, pack_void = lax.optimization_barrier((x_a, x_b, voidage))
    pack = pl.pallas_call(
        optional(pack_kernel, () if two_y else (4,)),
        out_shape=y_out + [f32(8, flat)] * 2,
        in_specs=[vmem] * 3,
        scratch_shapes=[pltpu.VMEM((flat, nz), jnp.float32)],
        compiler_params=PARAMS,
        name="pack",
    )
    *y_faces, z_a, z_b = pack(velocity, pressure, pack_void)
    near += [swap(y, "gy", k == 1) for k, y in enumerate(y_faces)]
    z_near = [swap(z_a, "gz"), swap(z_b, "gz", True)]

    cube = f32(nx, ny, nz)
    rate, scale, void_part = pl.pallas_call(
        drag_kernel,
        out_shape=[cube, cube, f32(1, nz)],
        in_specs=[vmem] * 3,
        compiler_params=PARAMS,
        name="drag",
    )(velocity, voidage, particle_vel)

    def whole(value):
        return pl.BlockSpec(value.shape, lambda i: (0,) * len(value.shape))

    def one(c):
        return pl.BlockSpec((1, nx, ny, nz), lambda i: (c, 0, 0, 0))

    def call(kernel, args, specs, outs, out_specs, **more):
        return pl.pallas_call(
            kernel,
            grid=(1,),
            in_specs=[whole(v) if spec is None else spec for v, spec in zip(args, specs)],
            out_shape=outs,
            out_specs=[whole(v) if spec is None else spec for v, spec in zip(outs, out_specs)],
            compiler_params=PARAMS,
            **more,
        )(*args)

    args = [forcing, velocity, pressure, voidage, particle_vel, rate, scale, void_part, *near, *z_near]
    face_rows = flat // nz
    tile = f32(-(-(face_rows + 2) // 8) * 8, nz)
    outs = [cube, f32(flat, nz), cube, tile, tile, tile, f32(flat, nz)]
    uz, flux_z, slope, fz_a, fz_b, sums, halo = call(
        optional(z_kernel, () if two_y else (11,)),
        args, [smem, None, None, None, one(2)] + [None] * (len(args) - 5), outs, [None] * len(outs),
    )
    gz_a = swap(fz_a, "gz")

    args = [velocity, pressure, voidage, particle_vel, rate, scale, flux_z, halo, *near]
    outs = [cube, cube] + [f32(nx, nz)] * len(y_faces)
    uy, div_yz, *fy = call(
        optional(y_kernel, () if two_y else (11, 15)),
        args, [None, None, None, one(1)] + [None] * (len(args) - 4),
        outs, [None] * len(outs),
    )
    fz_b, fy[0] = lax.optimization_barrier((fz_b, fy[0]))

    in_sums = lax.broadcasted_iota(jnp.int32, tile.shape, 0) >= face_rows

    def z_total(value):
        return jnp.where(in_sums, value, 0.0)

    def reduce_rest(total, axis):
        step = 2
        while counts[axis] > 4 and step < counts[axis]:
            swaps = [(i, i ^ step) for i in range(counts[axis])]
            total = total + lax.ppermute(total, axis, swaps)
            step *= 2
        return total

    def second(face, total, axis):
        got = swap(jnp.concatenate([face, total]), axis, True)
        if counts[axis] == 4:
            total = total + got[-tile.shape[0] :]
        return got, reduce_rest(total, axis)

    total = sums + z_total(gz_a)
    gz_b = swap(fz_b + total, "gz", True)

    args = [velocity, pressure, voidage, particle_vel, rate, scale, halo, div_yz, *near]
    outs = [cube, cube, f32(ny, nz), f32(ny, nz)]
    ux, div, fx_a, fx_b = call(
        optional(x_kernel, () if two_y else (11,)),
        args, [None, None, None, one(0)] + [None] * (len(args) - 4),
        outs, [None] * 4,
        scratch_shapes=[pltpu.VMEM((nx, ny, nz), jnp.float32)],
    )
    if counts["gz"] == 4:
        total = total + z_total(gz_b)
    total = reduce_rest(total, "gz")

    face, fx_a, fx_b = lax.optimization_barrier((fy[0], fx_a, fx_b))
    gy = [swap(jnp.concatenate([face, total]), "gy")]
    total = total + gy[0][-tile.shape[0] :]
    if two_y:
        got, total = second(fy[1], total, "gy")
        gy.append(got)

    vel_xy = pl.pallas_call(
        copy_kernel,
        out_shape=f32(3, nx, ny, nz),
        in_specs=[vmem] * 2,
        out_specs=any_space,
        scratch_shapes=[pltpu.SemaphoreType.DMA((2,))],
        compiler_params=PARAMS,
        name="copy_xy",
    )(ux, uy)
    fx_a, vel_xy = lax.optimization_barrier((fx_a, vel_xy))
    gx_a = swap(jnp.concatenate([fx_a, total]), "gx")
    total = total + gx_a[-tile.shape[0] :]
    args = [div, *gy, gz_a, gz_b]
    (div,) = call(
        optional(edge_kernel, () if two_y else (2,)),
        args, [None] * len(args), [cube], [None],
        scratch_shapes=[pltpu.VMEM((flat, nz), jnp.float32)],
    )
    fx_b, div = lax.optimization_barrier((fx_b, div))
    gx_b, total = second(fx_b, total, "gx")

    args = [forcing, target_flux, vel_xy, uz, div, slope, total, gx_a, gx_b]
    vel_new, source, forcing_new = call(
        functools.partial(finish_kernel, cells),
        args, [smem, smem, any_space] + [None] * (len(args) - 3),
        [f32(3, nx, ny, nz), cube, f32(1)], [one(2), None, smem],
        input_output_aliases={2: 0},
    )
    return vel_new, source, forcing_new


def solution(mesh):
    return jax.shard_map(
        local,
        mesh=mesh,
        in_specs=(
            P(None, "gx", "gy", "gz"),
            P("gx", "gy", "gz"),
            P("gx", "gy", "gz"),
            P(None, "gx", "gy", "gz"),
            P(),
            P(),
        ),
        out_specs=(P(None, "gx", "gy", "gz"), P("gx", "gy", "gz"), P()),
        check_vma=False,
    )
```
